16 devices in a mesh: dp: 16 (over z, y, x, core).
Axes of the slice: x: 2, y: 2, z: 2, core: 2. Of those that a mesh axis runs over, the one named last changes fastest.
Arguments:
- query_feat: bfloat16 [8192, 512], P('dp')
- item_feat: bfloat16 [8192, 512], P('dp')
- log_q: float32 [8192], P('dp')
- w_query_in: bfloat16 [512, 256], replicated
- w_query_out: bfloat16 [256, 128], replicated
- w_item_in: bfloat16 [512, 256], replicated
- w_item_out: bfloat16 [256, 128], replicated
Outputs:
- output 1: float32 [1], replicated
- output 2: float32 [512, 256], replicated
- output 3: float32 [256, 128], replicated
- output 4: float32 [512, 256], replicated
- output 5: float32 [256, 128], replicated
All inputs are finite; a program needn't handle non-finite values.
Results may differ from the reference program's by a relative error of at most 0.0074964.
Values are sent between devices in bfloat16 or wider.
A program may use at most 1 GiB of HBM per device.

```python
import jax
import jax.numpy as jnp
from jax import lax

GROUP_DEVICES = 16
ROWS_DEV = 512
FEAT_DIM = 512
HIDDEN_DIM = 256
EMBED_DIM = 128
GLOBAL_ROWS = GROUP_DEVICES * ROWS_DEV
POOL_SIZE = GLOBAL_ROWS // 4
BLOCK_ROWS = min(GLOBAL_ROWS, 256)
TEMPERATURE = 0.05
NORM_EPS = 1e-6


def setup_inputs(seed: int = 0) -> dict:
    base_key = jax.random.key(seed)
    keys_all = jax.random.split(base_key, 9)
    query_feat = jax.random.normal(keys_all[0], (GLOBAL_ROWS, FEAT_DIM), jnp.float32).astype(jnp.bfloat16)
    item_pool = jax.random.normal(keys_all[1], (POOL_SIZE, FEAT_DIM), jnp.float32)
    pick_a = jax.random.randint(keys_all[2], (GLOBAL_ROWS,), 0, POOL_SIZE)
    pick_b = jax.random.randint(keys_all[3], (GLOBAL_ROWS,), 0, POOL_SIZE)
    item_ids = (pick_a * pick_b) // POOL_SIZE
    item_feat = jnp.take(item_pool, item_ids, axis=0).astype(jnp.bfloat16)
    counts = jax.ops.segment_sum(jnp.ones((GLOBAL_ROWS,), jnp.float32), item_ids, num_segments=POOL_SIZE)
    log_q = jnp.log(jnp.take(counts, item_ids) / GLOBAL_ROWS) + 0.3 * jax.random.normal(keys_all[4], (GLOBAL_ROWS,), jnp.float32)
    w_query_in = (jax.random.normal(keys_all[5], (FEAT_DIM, HIDDEN_DIM), jnp.float32) * FEAT_DIM ** -0.5).astype(jnp.bfloat16)
    w_query_out = (jax.random.normal(keys_all[6], (HIDDEN_DIM, EMBED_DIM), jnp.float32) * HIDDEN_DIM ** -0.5).astype(jnp.bfloat16)
    w_item_in = (jax.random.normal(keys_all[7], (FEAT_DIM, HIDDEN_DIM), jnp.float32) * FEAT_DIM ** -0.5).astype(jnp.bfloat16)
    w_item_out = (jax.random.normal(keys_all[8], (HIDDEN_DIM, EMBED_DIM), jnp.float32) * HIDDEN_DIM ** -0.5).astype(jnp.bfloat16)
    return {'query_feat': query_feat, 'item_feat': item_feat, 'log_q': log_q, 'w_query_in': w_query_in, 'w_query_out': w_query_out, 'w_item_in': w_item_in, 'w_item_out': w_item_out}


def tower_forward(feat_rows, w_in, w_out):
    pre_act = jnp.dot(feat_rows, w_in, preferred_element_type=jnp.float32)
    hidden = jnp.maximum(pre_act, 0.0).astype(jnp.bfloat16)
    embed = jnp.dot(hidden, w_out, preferred_element_type=jnp.float32)
    inv_norm = lax.rsqrt(jnp.sum(embed * embed, axis=-1, keepdims=True) + NORM_EPS)
    return pre_act, hidden, inv_norm, embed * inv_norm


def tower_backward(feat_rows, w_out, pre_act, hidden, inv_norm, unit_vec, d_unit):
    d_embed = inv_norm * (d_unit - unit_vec * jnp.sum(unit_vec * d_unit, axis=-1, keepdims=True))
    d_embed_bf = d_embed.astype(jnp.bfloat16)
    grad_out = jnp.dot(hidden.T, d_embed_bf, preferred_element_type=jnp.float32)
    d_hidden = jnp.dot(d_embed_bf, w_out.T, preferred_element_type=jnp.float32)
    d_pre = jnp.where(pre_act > 0, d_hidden, 0.0).astype(jnp.bfloat16)
    grad_in = jnp.dot(feat_rows.T, d_pre, preferred_element_type=jnp.float32)
    return grad_in, grad_out


def softmax_grads(query_bf, items_bf, log_q):
    num_blocks = GLOBAL_ROWS // BLOCK_ROWS
    grad_scale = 1.0 / (TEMPERATURE * GLOBAL_ROWS)
    col_ids = jnp.arange(GLOBAL_ROWS)[None, :]
    query_blocks = query_bf.reshape(num_blocks, BLOCK_ROWS, EMBED_DIM)

    def block_step(d_item_acc, inputs):
        block_index, query_blk = inputs
        logits = jnp.dot(query_blk, items_bf.T, preferred_element_type=jnp.float32) / TEMPERATURE - log_q[None, :]
        row_ids = block_index * BLOCK_ROWS + jnp.arange(BLOCK_ROWS)[:, None]
        is_pos = row_ids == col_ids
        row_max = jnp.max(logits, axis=1, keepdims=True)
        log_norm = row_max + jnp.log(jnp.sum(jnp.exp(logits - row_max), axis=1, keepdims=True))
        pos_logit = jnp.sum(jnp.where(is_pos, logits, 0.0), axis=1, keepdims=True)
        prob_rows = jnp.exp(logits - log_norm)
        grad_logits = jnp.where(is_pos, prob_rows - 1.0, prob_rows).astype(jnp.bfloat16)
        d_query_blk = jnp.dot(grad_logits, items_bf, preferred_element_type=jnp.float32) * grad_scale
        d_item_acc = d_item_acc + jnp.dot(grad_logits.T, query_blk, preferred_element_type=jnp.float32)
        return d_item_acc, (jnp.sum(log_norm - pos_logit), d_query_blk)

    acc_init = jnp.zeros((GLOBAL_ROWS, EMBED_DIM), jnp.float32)
    d_item_acc, (loss_parts, d_query_blocks) = lax.scan(block_step, acc_init, (jnp.arange(num_blocks), query_blocks))
    return jnp.sum(loss_parts), d_query_blocks.reshape(GLOBAL_ROWS, EMBED_DIM), d_item_acc * grad_scale


def reference(query_feat, item_feat, log_q, w_query_in, w_query_out, w_item_in, w_item_out):
    q_pre, q_hidden, q_inv, q_unit = tower_forward(query_feat, w_query_in, w_query_out)
    v_pre, v_hidden, v_inv, v_unit = tower_forward(item_feat, w_item_in, w_item_out)
    loss_sum, d_query, d_item = softmax_grads(q_unit.astype(jnp.bfloat16), v_unit.astype(jnp.bfloat16), log_q)
    grad_query_in, grad_query_out = tower_backward(query_feat, w_query_out, q_pre, q_hidden, q_inv, q_unit, d_query)
    grad_item_in, grad_item_out = tower_backward(item_feat, w_item_out, v_pre, v_hidden, v_inv, v_unit, d_item)
    loss = jnp.reshape(loss_sum / GLOBAL_ROWS, (1,))
    return (loss, grad_query_in, grad_query_out, grad_item_in, grad_item_out)
```

```python
import jax
import jax.numpy as jnp
from jax import lax
from jax.experimental import pallas as pl
from jax.experimental.pallas import tpu as pltpu
from jax.sharding import PartitionSpec as P

MESH = pl.DeviceIdType.MESH
TEMPERATURE = 0.05
NORM_EPS = 1e-6
LOG2E = 1.4426950408889634
NDEV = 16
ROWS = 512
FEAT = 512
HID = 256
EMB = 128
TOTAL = NDEV * ROWS
GRAD_SCALE = 1.0 / (TEMPERATURE * TOTAL)
LOGIT_SCALE = LOG2E / TEMPERATURE
PARTS = ((0, 176), (176, 176), (352, 160))
ORDERS = ((1, 2, 4), (2, 4, 1), (4, 1, 2))
LEVELS = ((1, 2, 4), (6, 5, 3), (7,))
MSG = ROWS + 128
F32 = jnp.float32
BF16 = jnp.bfloat16


def dot_nn(a, b):
    return lax.dot_general(a, b, (((1,), (0,)), ((), ())), preferred_element_type=F32)


def dot_nt(a, b):
    return lax.dot_general(a, b, (((1,), (1,)), ((), ())), preferred_element_type=F32)


def dot_tn(a, b):
    return lax.dot_general(a, b, (((0,), (0,)), ((), ())), preferred_element_type=F32)


def kernel(qx, vx, lq, wqi, wqo, wvi, wvo,
           loss_out, gqi_out, gqo_out, gvi_out, gvo_out,
           uall, vall, lqall, brow, msgs, exps, lacc,
           a_q, a_v, h_q, h_v, u_q, u_v, r_q, r_v, invl, bcol, dacc,
           pi_q, po_q, pi_v, po_v, ri_q, ro_q, ri_v, ro_v,
           s_lq, m_lq, s_msg, m_msg,
           s_v, m_v, s_vd, m_vd, s_u, m_u, s_ud, m_ud,
           s_pair, m_pair, s_rs, m_rs, s_ag, m_ag, s_fw, m_fw):
    me = lax.axis_index("dp")
    core = me % 2
    bit_x, bit_y, bit_z = (me // 2) % 2, (me // 4) % 2, (me // 8) % 2
    step_x, step_y, step_z = 2 - 4 * bit_x, 4 - 8 * bit_y, 8 - 16 * bit_z
    partner = me + 1 - 2 * core
    chip = me // 2

    def dev(mask):
        return me + (mask % 2) * step_x + ((mask // 2) % 2) * step_y + (mask // 4) * step_z

    def dev_other(mask):
        return partner + (mask % 2) * step_x + ((mask // 2) % 2) * step_y + (mask // 4) * step_z

    def rcopy(src, dst, ssem, rsem, to):
        return pltpu.make_async_remote_copy(src_ref=src, dst_ref=dst, send_sem=ssem, recv_sem=rsem,
                                            device_id=(to,), device_id_type=MESH)

    pending = []

    def send(src, dst, ssem, rsem, to):
        copy = rcopy(src, dst, ssem, rsem, to)
        copy.start()
        pending.append(copy)

    def arrived(ref, rsem):
        rcopy(ref, ref, rsem, rsem, partner).wait_recv()

    others = [(me + k) % NDEV for k in range(1, NDEV)]

    barrier = pltpu.get_barrier_semaphore()
    for k in range(NDEV - 1):
        pl.semaphore_signal(barrier, inc=1, device_id=(others[k],), device_id_type=MESH)

    def tower_forward(x, w_in, w_out, a_ref, h_ref, u_ref, r_ref, all_ref):
        a = dot_nn(x[...], w_in[...])
        a_ref[...] = a
        h = jnp.maximum(a, 0.0).astype(BF16)
        h_ref[...] = h
        e = dot_nn(h, w_out[...])
        r = lax.rsqrt(jnp.sum(e * e, axis=-1, keepdims=True) + NORM_EPS)
        u = e * r
        u_ref[...] = u
        r_ref[...] = jnp.broadcast_to(r, (ROWS, EMB))
        all_ref[me] = u.astype(BF16)

    lqall[me] = lq[...]
    tower_forward(vx, wvi, wvo, a_v, h_v, u_v, r_v, vall)
    pl.semaphore_wait(barrier, NDEV - 1)

    for k in range(NDEV - 1):
        send(lq, lqall.at[me], s_lq.at[k], m_lq.at[k], others[k])

    def part_ref(ref, src, p):
        return ref.at[src, pl.ds(PARTS[p][0], PARTS[p][1]), :]

    def gather_own(ref, ss, ms, sd, md):
        send(ref.at[me], ref.at[me], sd.at[0], md.at[0], partner)
        for t in range(3):
            for p in range(3):
                d = ORDERS[p][t]
                send(part_ref(ref, me, p), part_ref(ref, me, p), ss.at[p, 0, t], ms.at[p, d], dev(d))

    def gather_level(ref, level, ss, ms, sd, md):
        jobs = []
        for p in range(3):
            for m in LEVELS[level]:
                top = max(t for t in range(3) if ORDERS[p][t] & m)
                jobs.append((top, p, m))
        for top, p, m in sorted(jobs):
            src = dev(m)
            arrived(part_ref(ref, src, p), ms.at[p, m])
            for t in range(top + 1, 3):
                d = ORDERS[p][t]
                send(part_ref(ref, src, p), part_ref(ref, src, p), ss.at[p, m, t], ms.at[p, m + d], dev(d))
        for m in LEVELS[level]:
            send(ref.at[dev(m)], ref.at[dev(m)], sd.at[m], md.at[m], partner)

    def gather_pair(ref, masks, md):
        for m in masks:
            arrived(ref.at[dev_other(m)], md.at[m])

    gather_own(vall, s_v, m_v, s_vd, m_vd)

    tower_forward(qx, wqi, wqo, a_q, h_q, u_q, r_q, uall)

    for k in range(NDEV - 1):
        src = (me + NDEV - 1 - k) % NDEV
        arrived(lqall.at[src], m_lq.at[k])
    shift = jnp.max(-lqall[...])
    brow[...] = (lqall[...] + shift) * LOG2E
    bcol[...] = jnp.broadcast_to((lq[...] + shift) * LOG2E, (EMB, ROWS)).T

    lacc[...] = jnp.zeros_like(lacc)

    def exp_block(b):
        s = dot_nt(uall[me], vall[b])
        e = jnp.exp2(s * LOGIT_SCALE - brow[b])
        exps[b] = e
        part = e[:, 0:128] + e[:, 128:256] + (e[:, 256:384] + e[:, 384:512])
        lacc[...] += part

    exp_block(me)
    gather_pair(vall, (0,), m_vd)
    exp_block(partner)

    def exp_level(masks):
        for m in masks:
            exp_block(dev(m))
        gather_pair(vall, masks, m_vd)
        for m in masks:
            exp_block(dev_other(m))

    gather_level(vall, 0, s_v, m_v, s_vd, m_vd)
    gather_own(uall, s_u, m_u, s_ud, m_ud)

    def exp_pair_loop(level):
        def body(i, _):
            m = LEVELS[level][0] if len(LEVELS[level]) == 1 else (i * (i + 1) // 2 + 1)
            if level == 1:
                m = 7 - m
            exp_block(dev(m))
            return 0
        lax.fori_loop(0, len(LEVELS[level]), body, 0)
        gather_pair(vall, LEVELS[level], m_vd)

        def body2(i, _):
            m = LEVELS[level][0] if len(LEVELS[level]) == 1 else (i * (i + 1) // 2 + 1)
            if level == 1:
                m = 7 - m
            exp_block(dev_other(m))
            return 0
        lax.fori_loop(0, len(LEVELS[level]), body2, 0)

    exp_pair_loop(0)
    gather_level(vall, 1, s_v, m_v, s_vd, m_vd)
    exp_pair_loop(1)
    gather_level(vall, 2, s_v, m_v, s_vd, m_vd)
    gather_level(uall, 0, s_u, m_u, s_ud, m_ud)
    exp_pair_loop(2)

    acc = lacc[...]
    l_row = jnp.sum(acc.T, axis=0, keepdims=True)
    invl[...] = jnp.broadcast_to(1.0 / jnp.sum(acc, axis=1, keepdims=True), (ROWS, EMB))
    pos = (uall[me].astype(F32) * vall[me].astype(F32)).T
    pos_row = jnp.sum(pos, axis=0, keepdims=True)
    loss_row = jnp.log(l_row) + ((shift + lq[...]) - pos_row * (1.0 / TEMPERATURE))
    loss_part = loss_row[:, 0:128] + loss_row[:, 128:256] + (loss_row[:, 256:384] + loss_row[:, 384:512])
    msgs[me, :, 0:ROWS] = 1.0 / l_row
    msgs[me, :, ROWS:MSG] = loss_part

    gather_level(uall, 1, s_u, m_u, s_ud, m_ud)
    for k in range(NDEV - 1):
        send(msgs.at[me], msgs.at[me], s_msg.at[k], m_msg.at[k], others[k])

    eye = (lax.broadcasted_iota(jnp.int32, (ROWS, ROWS), 0)
           == lax.broadcasted_iota(jnp.int32, (ROWS, ROWS), 1))

    def wide(col):
        return jnp.concatenate([col, col, col, col], axis=1)

    g_own = jnp.where(eye, exps[me] * wide(invl[...]) - 1.0, exps[me] * wide(invl[...])).astype(BF16)
    dacc[...] = dot_nn(g_own, vall[me])

    def du_step(i, _):
        b = (me + i) % NDEV
        g = (exps[b] * wide(invl[...])).astype(BF16)
        dacc[...] += dot_nn(g, vall[b])
        return 0
    lax.fori_loop(1, NDEV, du_step, 0)

    gather_level(uall, 2, s_u, m_u, s_ud, m_ud)

    def tower_backward(x, w_out, a_ref, h_ref, u_ref, r_ref, gi, go):
        du = dacc[...] * GRAD_SCALE
        u = u_ref[...]
        de = (r_ref[...] * (du - u * jnp.sum(u * du, axis=-1, keepdims=True))).astype(BF16)
        go[...] = dot_tn(h_ref[...], de)
        dh = dot_nt(de, w_out[...])
        da = jnp.where(a_ref[...] > 0, dh, 0.0).astype(BF16)
        gi[...] = dot_tn(x[...], da)

    def half_in(c):
        return pl.ds(pl.multiple_of(c * 256, 256), 256)

    def half_out(c):
        return pl.ds(pl.multiple_of(c * 128, 128), 128)

    def shard_in(c, k):
        return pl.ds(pl.multiple_of(c * 256 + k * 32, 32), 32)

    def shard_out(c, k):
        return pl.ds(pl.multiple_of(c * 128 + k * 16, 16), 16)

    def pair_start(t, gi, go, pi, po):
        send(gi.at[half_in(1 - core), :], pi, s_pair.at[t, 0], m_pair.at[t, 0], partner)
        send(go.at[half_out(1 - core), :], po, s_pair.at[t, 1], m_pair.at[t, 1], partner)

    def pair_finish(t, gi, go, pi, po, ri, ro):
        arrived(pi, m_pair.at[t, 0])
        arrived(po, m_pair.at[t, 1])
        pi[...] = pi[...] + gi[half_in(core), :]
        po[...] = po[...] + go[half_out(core), :]
        for m in range(7, 0, -1):
            to = dev(m)
            k = to // 2
            send(pi.at[pl.ds(pl.multiple_of(k * 32, 32), 32), :], ri.at[chip], s_rs.at[t, 0, m], m_rs.at[t, 0, m], to)
            send(po.at[pl.ds(pl.multiple_of(k * 16, 16), 16), :], ro.at[chip], s_rs.at[t, 1, m], m_rs.at[t, 1, m], to)

    def rs_finish(t, gi_o, go_o, pi, po, ri, ro, fi, fo):
        for m in range(1, 8):
            k = dev(m) // 2
            arrived(ri.at[k], m_rs.at[t, 0, m])
            arrived(ro.at[k], m_rs.at[t, 1, m])
        ti = pi[pl.ds(pl.multiple_of(chip * 32, 32), 32), :]
        to_ = po[pl.ds(pl.multiple_of(chip * 16, 16), 16), :]
        for m in range(1, 8):
            k = dev(m) // 2
            ti = ti + ri[k]
            to_ = to_ + ro[k]
        gi_o[shard_in(core, chip), :] = ti
        go_o[shard_out(core, chip), :] = to_
        for m in range(7, 0, -1):
            to = dev(m)
            for n, ref in ((0, gi_o.at[shard_in(core, chip), :]), (1, go_o.at[shard_out(core, chip), :])):
                send(ref, ref, s_ag.at[t, n, m], m_ag.at[t, n, m], to)

    def ag_forward(t, gi_o, go_o):
        for m in range(1, 8):
            k = dev(m) // 2
            arrived(gi_o.at[shard_in(core, k), :], m_ag.at[t, 0, m])
            arrived(go_o.at[shard_out(core, k), :], m_ag.at[t, 1, m])
        send(gi_o.at[half_in(core), :], gi_o.at[half_in(core), :], s_fw.at[t, 0], m_fw.at[t, 0], partner)
        send(go_o.at[half_out(core), :], go_o.at[half_out(core), :], s_fw.at[t, 1], m_fw.at[t, 1], partner)

    def ag_finish(t, gi_o, go_o):
        arrived(gi_o.at[half_in(1 - core), :], m_fw.at[t, 0])
        arrived(go_o.at[half_out(1 - core), :], m_fw.at[t, 1])

    def q_part(body):
        return body

    def run(gi_q, go_q, gi_v, go_v):
        tower_backward(qx, wqo, a_q, h_q, u_q, r_q, gi_q, go_q)
        pair_start(0, gi_q, go_q, pi_q, po_q)

        for k in range(NDEV - 1):
            src = (me + NDEV - 1 - k) % NDEV
            arrived(msgs.at[src], m_msg.at[k])
        total = msgs[0, :, ROWS:MSG]
        for b in range(1, NDEV):
            total = total + msgs[b, :, ROWS:MSG]
        loss_out[...] = jnp.broadcast_to(jnp.sum(total, axis=1, keepdims=True) * (1.0 / TOTAL), (1, 128))

        gather_pair(uall, range(8), m_ud)
        pair_finish(0, gi_q, go_q, pi_q, po_q, ri_q, ro_q)

        def dv_block(b, own):
            s = dot_nt(vall[me], uall[b])
            p = jnp.exp2(s * LOGIT_SCALE - wide(bcol[...])) * msgs[b, :, 0:ROWS]
            if own:
                p = jnp.where(eye, p - 1.0, p)
            return dot_nn(p.astype(BF16), uall[b])

        dacc[...] = dv_block(me, True)

        def dv_step(i, _):
            b = (me + i) % NDEV
            dacc[...] += dv_block(b, False)
            return 0
        lax.fori_loop(1, 9, dv_step, 0)
        rs_finish(0, gqi_out, gqo_out, pi_q, po_q, ri_q, ro_q, None, None)
        lax.fori_loop(9, NDEV, dv_step, 0)

        tower_backward(vx, wvo, a_v, h_v, u_v, r_v, gi_v, go_v)
        pair_start(1, gi_v, go_v, pi_v, po_v)
        ag_forward(0, gqi_out, gqo_out)
        pair_finish(1, gi_v, go_v, pi_v, po_v, ri_v, ro_v)
        rs_finish(1, gvi_out, gvo_out, pi_v, po_v, ri_v, ro_v, None, None)
        ag_finish(0, gqi_out, gqo_out)
        ag_forward(1, gvi_out, gvo_out)
        ag_finish(1, gvi_out, gvo_out)
        for copy in pending:
            copy.wait_send()

    pl.run_scoped(run, pltpu.VMEM((FEAT, HID), F32), pltpu.VMEM((HID, EMB), F32),
                  pltpu.VMEM((FEAT, HID), F32), pltpu.VMEM((HID, EMB), F32))


def solution(mesh):
    vmem = pl.BlockSpec(memory_space=pltpu.VMEM)
    dma = pltpu.SemaphoreType.DMA

    def local_step(query_feat, item_feat, log_q, w_query_in, w_query_out, w_item_in, w_item_out):
        shape = jax.ShapeDtypeStruct
        loss, gqi, gqo, gvi, gvo = pl.pallas_call(
            kernel,
            out_shape=(shape((1, 128), F32), shape((FEAT, HID), F32), shape((HID, EMB), F32),
                       shape((FEAT, HID), F32), shape((HID, EMB), F32)),
            in_specs=[vmem] * 7,
            out_specs=(vmem,) * 5,
            scratch_shapes=[
                pltpu.VMEM((NDEV, ROWS, EMB), BF16), pltpu.VMEM((NDEV, ROWS, EMB), BF16),
                pltpu.VMEM((NDEV, 1, ROWS), F32), pltpu.VMEM((NDEV, 1, ROWS), F32),
                pltpu.VMEM((NDEV, 1, MSG), F32),
                pltpu.VMEM((NDEV, ROWS, ROWS), F32), pltpu.VMEM((ROWS, EMB), F32),
                pltpu.VMEM((ROWS, HID), F32), pltpu.VMEM((ROWS, HID), F32),
                pltpu.VMEM((ROWS, HID), BF16), pltpu.VMEM((ROWS, HID), BF16),
                pltpu.VMEM((ROWS, EMB), F32), pltpu.VMEM((ROWS, EMB), F32),
                pltpu.VMEM((ROWS, EMB), F32), pltpu.VMEM((ROWS, EMB), F32),
                pltpu.VMEM((ROWS, EMB), F32), pltpu.VMEM((ROWS, EMB), F32), pltpu.VMEM((ROWS, EMB), F32),
                pltpu.VMEM((256, HID), F32), pltpu.VMEM((128, EMB), F32),
                pltpu.VMEM((256, HID), F32), pltpu.VMEM((128, EMB), F32),
                pltpu.VMEM((8, 32, HID), F32), pltpu.VMEM((8, 16, EMB), F32),
                pltpu.VMEM((8, 32, HID), F32), pltpu.VMEM((8, 16, EMB), F32),
                dma((15,)), dma((15,)), dma((15,)), dma((15,)),
                dma((3, 8, 3)), dma((3, 8)), dma((8,)), dma((8,)),
                dma((3, 8, 3)), dma((3, 8)), dma((8,)), dma((8,)),
                dma((2, 2)), dma((2, 2)), dma((2, 2, 8)), dma((2, 2, 8)),
                dma((2, 2, 8)), dma((2, 2, 8)), dma((2, 2)), dma((2, 2)),
            ],
            compiler_params=pltpu.CompilerParams(collective_id=0, has_side_effects=True,
                                                 vmem_limit_bytes=62 * 1024 * 1024),
            name="step",
        )(query_feat, item_feat, log_q.reshape(1, ROWS), w_query_in, w_query_out, w_item_in, w_item_out)
        return loss[0, 0:1], gqi, gqo, gvi, gvo

    return jax.shard_map(local_step, mesh=mesh, in_specs=(P('dp', None), P('dp', None), P('dp'), P(), P(), P(), P()), out_specs=(P(), P(), P(), P(), P()), check_vma=False)
```

```python
import jax
import jax.numpy as jnp
from jax import lax
from jax.experimental import pallas as pl
from jax.experimental.pallas import tpu as pltpu
from jax.sharding import PartitionSpec as P

MESH = pl.DeviceIdType.MESH
TEMPERATURE = 0.05
NORM_EPS = 1e-6
LOG2E = 1.4426950408889634
NDEV = 16
ROWS = 512
FEAT = 512
HID = 256
EMB = 128
PACK = FEAT + HID // 2
HALF = PACK // 2
SHARD = HALF // 8
TOTAL = NDEV * ROWS
GRAD_SCALE = 1.0 / (TEMPERATURE * TOTAL)
LOGIT_SCALE = LOG2E / TEMPERATURE
PARTS = ((0, 176), (176, 176), (352, 160))
ORDERS = ((1, 2, 4), (2, 4, 1), (4, 1, 2), (1, 2, 4))
LEVELS = ((1, 2, 4), (6, 5, 3), (7,))
MSG = ROWS + 128
F32 = jnp.float32
BF16 = jnp.bfloat16


def dot_nn(a, b):
    return lax.dot_general(a, b, (((1,), (0,)), ((), ())), preferred_element_type=F32)


def dot_nt(a, b):
    return lax.dot_general(a, b, (((1,), (1,)), ((), ())), preferred_element_type=F32)


def dot_tn(a, b):
    return lax.dot_general(a, b, (((0,), (0,)), ((), ())), preferred_element_type=F32)


def wide(col):
    return jnp.concatenate([col, col, col, col], axis=1)


def kernel(qx_h, vx_h, lq_h, wqi_h, wqo_h, wvi_h, wvo_h,
           loss_out, gq_out, gv_out,
           qx, vx, wqi, wqo, wvi, wvo, s_in,
           uall, vall, lqall, cmax, crun, msgs, exps, lacc,
           a_q, a_v, h_q, h_v, u_q, u_v, r_q, r_v, invl, bcol, dacc,
           gp_q, gp_v, pp_q, pp_v, rr_q, rr_v,
           s_msg, m_msg,
           s_v, m_v, s_vd, m_vd, s_ld, m_ld, s_u, m_u, s_ud, m_ud,
           s_pair, m_pair, s_rs, m_rs, s_ag, m_ag, s_fw, m_fw):
    me = lax.axis_index("dp")
    core = me % 2
    bit_x, bit_y, bit_z = (me // 2) % 2, (me // 4) % 2, (me // 8) % 2
    step_x, step_y, step_z = 2 - 4 * bit_x, 4 - 8 * bit_y, 8 - 16 * bit_z
    partner = me + 1 - 2 * core
    chip = me // 2

    def dev(mask):
        return me + (mask % 2) * step_x + ((mask // 2) % 2) * step_y + (mask // 4) * step_z

    def dev_other(mask):
        return partner + (mask % 2) * step_x + ((mask // 2) % 2) * step_y + (mask // 4) * step_z

    def rcopy(src, dst, ssem, rsem, to):
        return pltpu.make_async_remote_copy(src_ref=src, dst_ref=dst, send_sem=ssem, recv_sem=rsem,
                                            device_id=(to,), device_id_type=MESH)

    pending = []

    def send(src, dst, ssem, rsem, to):
        copy = rcopy(src, dst, ssem, rsem, to)
        copy.start()
        pending.append(copy)

    def arrived(ref, rsem):
        rcopy(ref, ref, rsem, rsem, partner).wait_recv()

    others = [(me + k) % NDEV for k in range(1, NDEV)]

    loads = [pltpu.make_async_copy(src, dst, s_in.at[i]) for i, (src, dst) in enumerate((
        (vx_h, vx), (wvi_h, wvi), (wvo_h, wvo), (lq_h, lqall.at[me]), (qx_h, qx), (wqi_h, wqi), (wqo_h, wqo)))]
    for load in loads:
        load.start()
    barrier = pltpu.get_barrier_semaphore()
    for to in (partner, dev(1), dev(2), dev(4)):
        pl.semaphore_signal(barrier, inc=1, device_id=(to,), device_id_type=MESH)

    def tower_forward(x, w_in, w_out, a_ref, h_ref, u_ref, r_ref, all_ref):
        a = dot_nn(x[...], w_in[...])
        a_ref[...] = a
        h = jnp.maximum(a, 0.0).astype(BF16)
        h_ref[...] = h
        e = dot_nn(h, w_out[...])
        r = lax.rsqrt(jnp.sum(e * e, axis=-1, keepdims=True) + NORM_EPS)
        u = e * r
        u_ref[...] = u
        r_ref[...] = jnp.broadcast_to(r, (ROWS, EMB))
        all_ref[me] = u.astype(BF16)

    for load in loads[:4]:
        load.wait()
    tower_forward(vx, wvi, wvo, a_v, h_v, u_v, r_v, vall)
    pl.semaphore_wait(barrier, 4)

    def part_ref(ref, src, p):
        if p == 3:
            return lqall.at[src]
        return ref.at[src, pl.ds(PARTS[p][0], PARTS[p][1]), :]

    def send_part(ref, src, p, m, t, ss, ms):
        d = ORDERS[p][t]
        send(part_ref(ref, src, p), part_ref(ref, src, p), ss.at[p, m, t], ms.at[p, m + d], dev(d))

    def gather_own(ref, ts, ps, ss, ms):
        for t in ts:
            for p in ps:
                send_part(ref, me, p, 0, t, ss, ms)

    def level_jobs(level, ps):
        jobs = []
        for p in ps:
            for m in LEVELS[level]:
                top = max(t for t in range(3) if ORDERS[p][t] & m)
                jobs.append((top, p, m))
        return sorted(jobs)

    def gather_jobs(ref, jobs, ss, ms):
        for top, p, m in jobs:
            src = dev(m)
            arrived(part_ref(ref, src, p), ms.at[p, m])
            for t in range(top + 1, 3):
                send_part(ref, src, p, m, t, ss, ms)

    def pair_send(ref, masks, sd, md):
        for m in masks:
            send(ref.at[dev(m)], ref.at[dev(m)], sd.at[m], md.at[m], partner)

    def pair_wait(ref, masks, md):
        for m in masks:
            arrived(ref.at[dev_other(m)], md.at[m])

    VP, UP = (3, 0, 1, 2), (0, 1, 2)
    pair_send(lqall, (0,), s_ld, m_ld)
    pair_send(vall, (0,), s_vd, m_vd)
    gather_own(vall, (0, 1, 2), VP, s_v, m_v)

    for load in loads[4:]:
        load.wait()
    tower_forward(qx, wqi, wqo, a_q, h_q, u_q, r_q, uall)
    pair_send(uall, (0,), s_ud, m_ud)

    crun[...] = jnp.broadcast_to(jnp.max(-lqall[me], axis=1, keepdims=True), (1, 128))
    lacc[...] = jnp.zeros_like(lacc)

    def exp_block(b):
        lq_b = lqall[b]
        c_b = jnp.max(-lq_b, axis=1, keepdims=True)
        cmax[b] = jnp.broadcast_to(c_b, (1, 128))
        s = dot_nt(uall[me], vall[b])
        e = jnp.exp2(s * LOGIT_SCALE - (lq_b + c_b) * LOG2E)
        exps[b] = e
        part = e[:, 0:128] + e[:, 128:256] + (e[:, 256:384] + e[:, 384:512])
        c_old = crun[...]
        c_new = jnp.maximum(c_old, cmax[b])
        lacc[...] = lacc[...] * jnp.exp2((c_old - c_new) * LOG2E) + part * jnp.exp2((cmax[b] - c_new) * LOG2E)
        crun[...] = c_new

    exp_block(me)
    pair_wait(lqall, (0,), m_ld)
    pair_wait(vall, (0,), m_vd)
    exp_block(partner)

    L0, L1, L2 = LEVELS
    gather_jobs(vall, level_jobs(0, VP), s_v, m_v)
    gather_own(uall, (0,), UP, s_u, m_u)
    pair_send(lqall, L0, s_ld, m_ld)
    pair_send(vall, L0, s_vd, m_vd)
    for m in L0:
        exp_block(dev(m))
    gather_jobs(vall, level_jobs(1, VP), s_v, m_v)
    gather_own(uall, (1, 2), UP, s_u, m_u)
    pair_send(lqall, L1, s_ld, m_ld)
    pair_send(vall, L1, s_vd, m_vd)
    pair_wait(lqall, L0, m_ld)
    pair_wait(vall, L0, m_vd)
    for m in L0:
        exp_block(dev_other(m))
    u_jobs = level_jobs(0, UP)
    gather_jobs(uall, u_jobs[:3], s_u, m_u)
    for m in L1:
        exp_block(dev(m))
    gather_jobs(vall, level_jobs(2, VP), s_v, m_v)
    pair_send(lqall, L2, s_ld, m_ld)
    pair_send(vall, L2, s_vd, m_vd)
    gather_jobs(uall, u_jobs[3:], s_u, m_u)
    pair_send(uall, L0, s_ud, m_ud)
    pair_wait(lqall, L1, m_ld)
    pair_wait(vall, L1, m_vd)
    for m in L1:
        exp_block(dev_other(m))
    exp_block(dev(7))
    pair_wait(lqall, L2, m_ld)
    pair_wait(vall, L2, m_vd)
    exp_block(dev_other(7))

    acc = lacc[...]
    shift = crun[0:1, 0:1]
    lq_own = lqall[me]
    l_row = jnp.sum(acc.T, axis=0, keepdims=True)
    pos = (uall[me].astype(F32) * vall[me].astype(F32)).T
    pos_row = jnp.sum(pos, axis=0, keepdims=True)
    loss_row = jnp.log(l_row) + ((shift + lq_own) - pos_row * (1.0 / TEMPERATURE))
    loss_part = loss_row[:, 0:128] + loss_row[:, 128:256] + (loss_row[:, 256:384] + loss_row[:, 384:512])
    msgs[me, :, 0:ROWS] = 1.0 / l_row
    msgs[me, :, ROWS:MSG] = loss_part
    gather_jobs(uall, level_jobs(1, UP), s_u, m_u)
    pair_send(uall, L1, s_ud, m_ud)
    for k in range(NDEV - 1):
        send(msgs.at[me], msgs.at[me], s_msg.at[k], m_msg.at[k], others[k])
    invl[...] = jnp.broadcast_to(1.0 / jnp.sum(acc, axis=1, keepdims=True), (ROWS, EMB))
    bcol[...] = jnp.broadcast_to((lq_own + shift) * LOG2E, (EMB, ROWS)).T

    eye = (lax.broadcasted_iota(jnp.int32, (ROWS, ROWS), 0)
           == lax.broadcasted_iota(jnp.int32, (ROWS, ROWS), 1))

    def prob_block(b):
        return exps[b] * wide(invl[...] * jnp.exp2((cmax[b] - crun[...]) * LOG2E))

    p_own = prob_block(me)
    dacc[...] = dot_nn(jnp.where(eye, p_own - 1.0, p_own).astype(BF16), vall[me])

    def du_step(i, _):
        total = dacc[...]
        for j in range(3):
            b = (me + 3 * i + j + 1) % NDEV
            total = total + dot_nn(prob_block(b).astype(BF16), vall[b])
        dacc[...] = total
        return 0
    lax.fori_loop(0, 3, du_step, 0)
    gather_jobs(uall, level_jobs(2, UP), s_u, m_u)
    pair_send(uall, L2, s_ud, m_ud)
    lax.fori_loop(3, 5, du_step, 0)

    def tower_backward(x, w_out, a_ref, h_ref, u_ref, r_ref, g):
        du = dacc[...] * GRAD_SCALE
        u = u_ref[...]
        de = (r_ref[...] * (du - u * jnp.sum(u * du, axis=-1, keepdims=True))).astype(BF16)
        go = dot_tn(h_ref[...], de)
        g[FEAT:PACK, 0:EMB] = go[0:128]
        g[FEAT:PACK, EMB:HID] = go[128:256]
        dh = dot_nt(de, w_out[...])
        da = jnp.where(a_ref[...] > 0, dh, 0.0).astype(BF16)
        g[0:FEAT, :] = dot_tn(x[...], da)

    def half(c):
        return pl.ds(pl.multiple_of(c * HALF, 8), HALF)

    def shard(c, k):
        return pl.ds(pl.multiple_of(c * HALF + k * SHARD, 8), SHARD)

    NEAR = (1, 2, 4, 3, 5, 6, 7)

    def pair_start(t, g, pp):
        send(g.at[half(1 - core), :], pp, s_pair.at[t], m_pair.at[t], partner)

    def pair_finish(t, g, pp, rr):
        arrived(pp, m_pair.at[t])
        pp[...] = pp[...] + g[half(core), :]
        for m in reversed(NEAR):
            to = dev(m)
            k = to // 2
            send(pp.at[pl.ds(pl.multiple_of(k * SHARD, 8), SHARD), :], rr.at[chip], s_rs.at[t, m], m_rs.at[t, m], to)

    def rs_finish(t, out, pp, rr):
        total = pp[pl.ds(pl.multiple_of(chip * SHARD, 8), SHARD), :]
        for m in NEAR:
            k = dev(m) // 2
            arrived(rr.at[k], m_rs.at[t, m])
            total = total + rr[k]
        out[shard(core, chip), :] = total
        ref = out.at[shard(core, chip), :]
        for m in reversed(NEAR):
            send(ref, ref, s_ag.at[t, m], m_ag.at[t, m], dev(m))
        send(ref, ref, s_fw.at[t, 0], m_fw.at[t, 0], partner)

    def ag_forward(t, out):
        for m in NEAR:
            ref = out.at[shard(core, dev(m) // 2), :]
            arrived(ref, m_ag.at[t, m])
            send(ref, ref, s_fw.at[t, m], m_fw.at[t, m], partner)

    def ag_finish(t, out):
        for m in (0,) + NEAR:
            arrived(out.at[shard(1 - core, dev(m) // 2), :], m_fw.at[t, m])

    tower_backward(qx, wqo, a_q, h_q, u_q, r_q, gp_q)
    pair_start(0, gp_q, pp_q)

    for k in range(NDEV - 1):
        src = (me + NDEV - 1 - k) % NDEV
        arrived(msgs.at[src], m_msg.at[k])
    total = msgs[0, :, ROWS:MSG]
    for b in range(1, NDEV):
        total = total + msgs[b, :, ROWS:MSG]
    loss_out[...] = jnp.broadcast_to(jnp.sum(total, axis=1, keepdims=True) * (1.0 / TOTAL), (1, 128))

    def dv_block(b, own):
        s = dot_nt(vall[me], uall[b])
        p = jnp.exp2(s * LOGIT_SCALE - wide(bcol[...])) * msgs[b, :, 0:ROWS]
        if own:
            p = jnp.where(eye, p - 1.0, p)
        return dot_nn(p.astype(BF16), uall[b])

    dacc[...] = dv_block(me, True)
    pair_finish(0, gp_q, pp_q, rr_q)
    pair_wait(uall, (0,) + NEAR, m_ud)

    def dv_step(i, _):
        total = dacc[...]
        for j in range(3):
            total = total + dv_block((me + 3 * i + j + 1) % NDEV, False)
        dacc[...] = total
        return 0
    lax.fori_loop(0, 3, dv_step, 0)
    rs_finish(0, gq_out, pp_q, rr_q)
    lax.fori_loop(3, 5, dv_step, 0)

    tower_backward(vx, wvo, a_v, h_v, u_v, r_v, gp_v)
    pair_start(1, gp_v, pp_v)
    ag_forward(0, gq_out)
    pair_finish(1, gp_v, pp_v, rr_v)
    ag_finish(0, gq_out)
    rs_finish(1, gv_out, pp_v, rr_v)
    ag_forward(1, gv_out)
    ag_finish(1, gv_out)
    for copy in pending:
        copy.wait_send()


def finish(loss, gq, gv, loss_out, gqi, gqo, gvi, gvo, sem):
    copies = []
    for i, (g, gi, go) in enumerate(((gq, gqi, gqo), (gv, gvi, gvo))):
        copies.append(pltpu.make_async_copy(g.at[0:FEAT, :], gi, sem.at[i, 0]))
        copies.append(pltpu.make_async_copy(g.at[FEAT:PACK, 0:EMB], go.at[0:128, :], sem.at[i, 1]))
        copies.append(pltpu.make_async_copy(g.at[FEAT:PACK, EMB:HID], go.at[128:256, :], sem.at[i, 2]))
    for copy in copies:
        copy.start()
    loss_out[0] = loss[0, 0]
    for copy in copies:
        copy.wait()


def solution(mesh):
    vmem = pl.BlockSpec(memory_space=pltpu.VMEM)
    smem = pl.BlockSpec(memory_space=pltpu.SMEM)
    hbm = pl.BlockSpec(memory_space=pltpu.HBM)
    anym = pl.BlockSpec(memory_space=pl.ANY)
    dma = pltpu.SemaphoreType.DMA
    V = pltpu.VMEM

    def local_step(query_feat, item_feat, log_q, w_query_in, w_query_out, w_item_in, w_item_out):
        shape = jax.ShapeDtypeStruct
        loss, gq, gv = pl.pallas_call(
            kernel,
            out_shape=(shape((1, 128), F32), shape((PACK, HID), F32), shape((PACK, HID), F32)),
            in_specs=[hbm] * 7,
            out_specs=(vmem, vmem, vmem),
            scratch_shapes=[
                V((ROWS, FEAT), BF16), V((ROWS, FEAT), BF16),
                V((FEAT, HID), BF16), V((HID, EMB), BF16), V((FEAT, HID), BF16), V((HID, EMB), BF16), dma((7,)),
                V((NDEV, ROWS, EMB), BF16), V((NDEV, ROWS, EMB), BF16),
                V((NDEV, 1, ROWS), F32), V((NDEV, 1, 128), F32), V((1, 128), F32),
                V((NDEV, 1, MSG), F32),
                V((NDEV, ROWS, ROWS), F32), V((ROWS, EMB), F32),
                V((ROWS, HID), F32), V((ROWS, HID), F32),
                V((ROWS, HID), BF16), V((ROWS, HID), BF16),
                V((ROWS, EMB), F32), V((ROWS, EMB), F32),
                V((ROWS, EMB), F32), V((ROWS, EMB), F32),
                V((ROWS, EMB), F32), V((ROWS, EMB), F32), V((ROWS, EMB), F32),
                V((PACK, HID), F32), V((PACK, HID), F32),
                V((HALF, HID), F32), V((HALF, HID), F32),
                V((8, SHARD, HID), F32), V((8, SHARD, HID), F32),
                dma((15,)), dma((15,)),
                dma((4, 8, 3)), dma((4, 8)), dma((8,)), dma((8,)), dma((8,)), dma((8,)),
                dma((3, 8, 3)), dma((3, 8)), dma((8,)), dma((8,)),
                dma((2,)), dma((2,)), dma((2, 8)), dma((2, 8)),
                dma((2, 8)), dma((2, 8)), dma((2, 8)), dma((2, 8)),
            ],
            compiler_params=pltpu.CompilerParams(collective_id=0, has_side_effects=True,
                                                 vmem_limit_bytes=48 * 1024 * 1024),
            name="step",
        )(*(pltpu.with_memory_space_constraint(x, pltpu.HBM) for x in (
            query_feat, item_feat, log_q.reshape(1, ROWS), w_query_in, w_query_out, w_item_in, w_item_out)))
        return pl.pallas_call(
            finish,
            out_shape=(shape((1,), F32), shape((FEAT, HID), F32), shape((HID, EMB), F32),
                       shape((FEAT, HID), F32), shape((HID, EMB), F32)),
            in_specs=[vmem, vmem, vmem],
            out_specs=(smem, hbm, hbm, hbm, hbm),
            scratch_shapes=[dma((2, 3))],
            compiler_params=pltpu.CompilerParams(vmem_limit_bytes=8 * 1024 * 1024),
            name="finish",
        )(loss, gq, gv)

    return jax.shard_map(local_step, mesh=mesh, in_specs=(P('dp', None), P('dp', None), P('dp'), P(), P(), P(), P()), out_specs=(P(), P(), P(), P(), P()), check_vma=False)
```

```python
import jax
import jax.numpy as jnp
from jax import lax
from jax.experimental import pallas as pl
from jax.experimental.pallas import tpu as pltpu
from jax.sharding import PartitionSpec as P

MESH = pl.DeviceIdType.MESH
TEMPERATURE = 0.05
NORM_EPS = 1e-6
LOG2E = 1.4426950408889634
NDEV = 16
ROWS = 512
FEAT = 512
HID = 256
EMB = 128
PACK = 2 * FEAT + HID
HALF = PACK // 2
SUM_BASE = (0, 192, 384)
SUM_ROWS = (192, 192, 256)
TOTAL = NDEV * ROWS
GRAD_SCALE = 1.0 / (TEMPERATURE * TOTAL)
LOGIT_SCALE = LOG2E / TEMPERATURE
PARTS = ((0, 176), (176, 176), (352, 160))
ORDERS = ((1, 2, 4), (2, 4, 1), (4, 1, 2), (1, 2, 4))
LEVELS = ((1, 2, 4), (6, 5, 3), (7,))
MSG = ROWS + 128
F32 = jnp.float32
BF16 = jnp.bfloat16


def dot_nn(a, b):
    return lax.dot_general(a, b, (((1,), (0,)), ((), ())), preferred_element_type=F32)


def dot_nt(a, b):
    return lax.dot_general(a, b, (((1,), (1,)), ((), ())), preferred_element_type=F32)


def dot_tn(a, b):
    return lax.dot_general(a, b, (((0,), (0,)), ((), ())), preferred_element_type=F32)


def wide(col):
    return jnp.concatenate([col, col, col, col], axis=1)


def kernel(qx_h, vx_h, lq_h, wqi_h, wqo_h, wvi_h, wvo_h,
           loss_out, gq_out, gv_out,
           qx, vx, wqi, wqo, wvi, wvo, s_in,
           uall, vall, lqall, crun, msgs, lacc, diag,
           a_q, a_v, h_q, h_v, u_q, u_v, r_q, r_v, invl, bcol, dacc,
           gp_q, gp_v, pp_q, pp_v, ra_q, ra_v, rb_q, rb_v,
           s_msg, m_msg,
           s_v, m_v, s_vd, m_vd, s_ld, m_ld, s_u, m_u, s_ud, m_ud,
           s_pair, m_pair, s_r1, m_r1, s_r2, m_r2, s_g1, m_g1, s_g2, m_g2, s_fw, m_fw):
    me = lax.axis_index("dp")
    core = me % 2
    bit_x, bit_y, bit_z = (me // 2) % 2, (me // 4) % 2, (me // 8) % 2
    step_x, step_y, step_z = 2 - 4 * bit_x, 4 - 8 * bit_y, 8 - 16 * bit_z
    partner = me + 1 - 2 * core
    chip = me // 2

    def dev(mask):
        return me + (mask % 2) * step_x + ((mask // 2) % 2) * step_y + (mask // 4) * step_z

    def dev_other(mask):
        return partner + (mask % 2) * step_x + ((mask // 2) % 2) * step_y + (mask // 4) * step_z

    def rcopy(src, dst, ssem, rsem, to):
        return pltpu.make_async_remote_copy(src_ref=src, dst_ref=dst, send_sem=ssem, recv_sem=rsem,
                                            device_id=(to,), device_id_type=MESH)

    pending = []

    def send(make):
        rcopy(*make()).start()
        pending.append(make)

    def arrived(ref, rsem):
        rcopy(ref, ref, rsem, rsem, partner).wait_recv()

    others = [(me + k) % NDEV for k in range(1, NDEV)]

    loads = [pltpu.make_async_copy(src, dst, s_in.at[i]) for i, (src, dst) in enumerate((
        (vx_h, vx), (wvi_h, wvi), (wvo_h, wvo), (lq_h, lqall.at[me]), (qx_h, qx), (wqi_h, wqi), (wqo_h, wqo)))]
    for load in loads:
        load.start()
    barrier = pltpu.get_barrier_semaphore()
    for to in (partner, dev(1), dev(2), dev(4)):
        pl.semaphore_signal(barrier, inc=1, device_id=(to,), device_id_type=MESH)

    def tower_forward(x, w_in, w_out, a_ref, h_ref, u_ref, r_ref, all_ref):
        a = dot_nn(x[...], w_in[...])
        a_ref[...] = a
        h = jnp.maximum(a, 0.0).astype(BF16)
        h_ref[...] = h
        e = dot_nn(h, w_out[...])
        r = lax.rsqrt(jnp.sum(e * e, axis=-1, keepdims=True) + NORM_EPS)
        u = e * r
        u_ref[...] = u
        r_ref[...] = jnp.broadcast_to(r, (ROWS, EMB))
        all_ref[me] = u.astype(BF16)

    for load in loads[:4]:
        load.wait()
    tower_forward(vx, wvi, wvo, a_v, h_v, u_v, r_v, vall)
    pl.semaphore_wait(barrier, 4)

    def part_ref(ref, src, p):
        if p == 3:
            return lqall.at[src]
        return ref.at[src, pl.ds(PARTS[p][0], PARTS[p][1]), :]

    def send_part(ref, p, m, t, ss, ms):
        d = ORDERS[p][t]
        send(lambda: (part_ref(ref, dev(m), p), part_ref(ref, dev(m), p), ss.at[p, m, t], ms.at[p, m + d], dev(d)))

    def gather_own(ref, ts, ps, ss, ms):
        for t in ts:
            for p in ps:
                send_part(ref, p, 0, t, ss, ms)

    def level_jobs(level, ps):
        jobs = []
        for p in ps:
            for m in LEVELS[level]:
                top = max(t for t in range(3) if ORDERS[p][t] & m)
                jobs.append((top, p, m))
        return sorted(jobs)

    def gather_jobs(ref, jobs, ss, ms):
        for top, p, m in jobs:
            src = dev(m)
            arrived(part_ref(ref, src, p), ms.at[p, m])
            for t in range(top + 1, 3):
                send_part(ref, p, m, t, ss, ms)

    def pair_send(ref, masks, sd, md):
        for m in masks:
            send(lambda m=m: (ref.at[dev(m)], ref.at[dev(m)], sd.at[m], md.at[m], partner))

    def pair_wait(ref, masks, md):
        for m in masks:
            arrived(ref.at[dev_other(m)], md.at[m])

    VP, UP = (3, 0, 1, 2), (0, 1, 2)
    pair_send(lqall, (0,), s_ld, m_ld)
    pair_send(vall, (0,), s_vd, m_vd)
    gather_own(vall, (0, 1, 2), VP, s_v, m_v)

    for load in loads[4:]:
        load.wait()
    tower_forward(qx, wqi, wqo, a_q, h_q, u_q, r_q, uall)
    pair_send(uall, (0,), s_ud, m_ud)

    eye = (lax.broadcasted_iota(jnp.int32, (ROWS, ROWS), 0)
           == lax.broadcasted_iota(jnp.int32, (ROWS, ROWS), 1))

    def block_shift(b):
        return jnp.max(-lqall[b], axis=1, keepdims=True)

    def exp_block(b, c):
        s = dot_nt(uall[me], vall[b])
        return jnp.exp2(s * LOGIT_SCALE - (lqall[b] + c) * LOG2E)

    def lane_sum(e):
        return e[:, 0:128] + e[:, 128:256] + (e[:, 256:384] + e[:, 384:512])

    def exp_group(blocks):
        c_old = crun[...]
        c = c_old
        for b in blocks:
            c = jnp.maximum(c, block_shift(b))
        crun[...] = c
        scale = jnp.exp2((c_old - c) * LOG2E)
        l_new, d_new = lacc[...] * scale, dacc[...] * scale
        for b in blocks:
            e = exp_block(b, c[:, 0:1])
            l_new = l_new + lane_sum(e)
            d_new = d_new + dot_nn(e.astype(BF16), vall[b])
        lacc[...], dacc[...] = l_new, d_new

    c_own = block_shift(me)
    crun[...] = jnp.broadcast_to(c_own, (1, 128))
    e_own = exp_block(me, c_own)
    lacc[...] = lane_sum(e_own)
    diag[...] = jnp.broadcast_to(jnp.sum(jnp.where(eye, e_own, 0.0), axis=1, keepdims=True), (ROWS, EMB))
    dacc[...] = dot_nn(jnp.where(eye, 0.0, e_own).astype(BF16), vall[me])
    pair_wait(lqall, (0,), m_ld)
    pair_wait(vall, (0,), m_vd)
    exp_group((partner,))

    L0, L1, L2 = LEVELS
    v0, v1, v2 = (level_jobs(k, VP) for k in range(3))
    u0, u1, u2 = (level_jobs(k, UP) for k in range(3))

    def group_devs(g):
        masks = [b + (g // 2) * (7 - 2 * b) for b in L0]
        return [dev(m) + (g % 2) * (partner - me) for m in masks]

    def exp_step(g, _):
        @pl.when(g == 0)
        def _():
            gather_jobs(vall, v0, s_v, m_v)
            pair_send(lqall, L0, s_ld, m_ld)
            pair_send(vall, L0, s_vd, m_vd)

        @pl.when(g == 1)
        def _():
            gather_jobs(vall, v1[:4], s_v, m_v)
            gather_own(uall, (0, 1, 2), UP, s_u, m_u)
            pair_wait(lqall, L0, m_ld)
            pair_wait(vall, L0, m_vd)

        @pl.when(g == 2)
        def _():
            gather_jobs(vall, v1[4:], s_v, m_v)
            pair_send(lqall, L1, s_ld, m_ld)
            pair_send(vall, L1, s_vd, m_vd)

        @pl.when(g == 3)
        def _():
            gather_jobs(vall, v2, s_v, m_v)
            pair_send(lqall, L2, s_ld, m_ld)
            pair_send(vall, L2, s_vd, m_vd)
            pair_wait(lqall, L1, m_ld)
            pair_wait(vall, L1, m_vd)

        exp_group(group_devs(g))
        return 0

    lax.fori_loop(0, 4, exp_step, 0)
    gather_jobs(uall, u0[:3], s_u, m_u)
    pair_wait(lqall, L2, m_ld)
    pair_wait(vall, L2, m_vd)
    exp_group((dev(7), dev_other(7)))

    acc = lacc[...]
    shift = crun[0:1, 0:1]
    lq_own = lqall[me]
    l_row = jnp.sum(acc.T, axis=0, keepdims=True)
    pos = (uall[me].astype(F32) * vall[me].astype(F32)).T
    pos_row = jnp.sum(pos, axis=0, keepdims=True)
    loss_row = jnp.log(l_row) + ((shift + lq_own) - pos_row * (1.0 / TEMPERATURE))
    loss_part = loss_row[:, 0:128] + loss_row[:, 128:256] + (loss_row[:, 256:384] + loss_row[:, 384:512])
    msgs[me, :, 0:ROWS] = 1.0 / l_row
    msgs[me, :, ROWS:MSG] = loss_part
    for k in range(NDEV - 1):
        send(lambda k=k: (msgs.at[me], msgs.at[me], s_msg.at[k], m_msg.at[k], others[k]))
    invl[...] = jnp.broadcast_to(1.0 / jnp.sum(acc, axis=1, keepdims=True), (ROWS, EMB))
    bcol[...] = jnp.broadcast_to((lq_own + shift) * LOG2E, (EMB, ROWS)).T

    p_own = diag[...] * jnp.exp2((c_own - crun[...]) * LOG2E) * invl[...]
    dacc[...] = dacc[...] * invl[...] + (p_own - 1.0).astype(BF16).astype(F32) * vall[me].astype(F32)
    gather_jobs(uall, u0[3:6], s_u, m_u)

    def tower_backward(x, w_out, a_ref, h_ref, u_ref, r_ref, g):
        du = dacc[...] * GRAD_SCALE
        u = u_ref[...]
        de = (r_ref[...] * (du - u * jnp.sum(u * du, axis=-1, keepdims=True))).astype(BF16)
        g[2 * FEAT:PACK, :] = dot_tn(h_ref[...], de)
        dh = dot_nt(de, w_out[...])
        da = jnp.where(a_ref[...] > 0, dh, 0.0).astype(BF16)
        gi = dot_tn(x[...], da)
        g[0:FEAT, :] = gi[:, 0:EMB]
        g[FEAT:2 * FEAT, :] = gi[:, EMB:HID]

    bit = {1: bit_x, 2: bit_y, 4: bit_z}
    PLANE = ((0, 1), (1, 0), (1, 1))

    def rows(base, size):
        return pl.ds(pl.multiple_of(base, 8), size)

    def slot(p, b0, b1, b2, count):
        eighth = SUM_ROWS[p] // 8
        return rows(SUM_BASE[p] + (b0 * 4 + b1 * 2 + b2) * eighth, count * eighth)

    def half(c):
        return rows(c * HALF, HALF)

    def out_slot(c, p, b0, b1, b2, count):
        eighth = SUM_ROWS[p] // 8
        return rows(c * HALF + SUM_BASE[p] + (b0 * 4 + b1 * 2 + b2) * eighth, count * eighth)

    def bits(p, f1=0, f2=0):
        d0, d1, d2 = ORDERS[p]
        b1 = bit[d1] if not f1 else 1 - bit[d1]
        b2 = bit[d2] if not f2 else 1 - bit[d2]
        return bit[d0], b1, b2

    def plane_dev(p, k):
        return dev(PLANE[k][0] * ORDERS[p][1] + PLANE[k][1] * ORDERS[p][2])

    def own_shard(out, p):
        return out.at[out_slot(core, p, *bits(p), 1), :]

    def plane_shard(out, p, k):
        return out.at[out_slot(core, p, *bits(p, *PLANE[k]), 1), :]

    def axis_half(out, p, far):
        b0 = bits(p)[0]
        return out.at[out_slot(core, p, 1 - b0 if far else b0, 0, 0, 4), :]

    def pair_start(t, g, pp):
        send(lambda: (g.at[half(1 - core), :], pp, s_pair.at[t], m_pair.at[t], partner))

    def pair_finish(t, g, pp, ra):
        arrived(pp, m_pair.at[t])
        pp[...] = pp[...] + g[half(core), :]
        for p in range(3):
            send(lambda p=p: (pp.at[slot(p, 1 - bits(p)[0], 0, 0, 4), :],
                              ra.at[pl.ds(SUM_BASE[p] // 2, SUM_ROWS[p] // 2), :],
                              s_r1.at[t, p], m_r1.at[t, p], dev(ORDERS[p][0])))

    def r1_finish(t, pp, ra, rb):
        for p in range(3):
            part = pl.ds(SUM_BASE[p] // 2, SUM_ROWS[p] // 2)
            arrived(ra.at[part, :], m_r1.at[t, p])
            b0, _, _ = bits(p)
            mine = slot(p, b0, 0, 0, 4)
            pp[mine, :] = pp[mine, :] + ra[part, :]
        for k in (2, 0, 1):
            for p in range(3):
                send(lambda p=p, k=k: (pp.at[slot(p, *bits(p, *PLANE[k]), 1), :],
                                       rb.at[k, pl.ds(SUM_BASE[p] // 8, SUM_ROWS[p] // 8), :],
                                       s_r2.at[t, p, k], m_r2.at[t, p, k], plane_dev(p, k)))

    def r2_finish(t, out, pp, rb):
        for p in range(3):
            part = pl.ds(SUM_BASE[p] // 8, SUM_ROWS[p] // 8)
            total = pp[slot(p, *bits(p), 1), :]
            for k in range(3):
                arrived(rb.at[k, part, :], m_r2.at[t, p, k])
                total = total + rb[k, part, :]
            mine = out_slot(core, p, *bits(p), 1)
            out[mine, :] = total
            for k in (2, 0, 1):
                send(lambda p=p, k=k: (own_shard(out, p), own_shard(out, p), s_g1.at[t, p, k], m_g1.at[t, p, k],
                                       plane_dev(p, k)))
            send(lambda p=p: (own_shard(out, p), own_shard(out, p), s_g2.at[t, p, 3], m_g2.at[t, p, 3],
                              dev(ORDERS[p][0])))

    def ag_plane(t, out):
        for k in range(3):
            for p in range(3):
                arrived(plane_shard(out, p, k), m_g1.at[t, p, k])
                send(lambda p=p, k=k: (plane_shard(out, p, k), plane_shard(out, p, k), s_g2.at[t, p, k],
                                       m_g2.at[t, p, k], dev(ORDERS[p][0])))
        for p in range(3):
            send(lambda p=p: (axis_half(out, p, 0), axis_half(out, p, 0), s_fw.at[t, p, 0], m_fw.at[t, p, 0], partner))

    def ag_axis(t, out):
        for p in range(3):
            b0, _, _ = bits(p)
            for k in range(4):
                f1, f2 = PLANE[k] if k < 3 else (0, 0)
                _, b1, b2 = bits(p, f1, f2)
                arrived(out.at[out_slot(core, p, 1 - b0, b1, b2, 1), :], m_g2.at[t, p, k])
            send(lambda p=p: (axis_half(out, p, 1), axis_half(out, p, 1), s_fw.at[t, p, 1], m_fw.at[t, p, 1], partner))

    def ag_finish(t, out):
        for p in range(3):
            b0, _, _ = bits(p)
            arrived(out.at[out_slot(1 - core, p, b0, 0, 0, 4), :], m_fw.at[t, p, 0])
            arrived(out.at[out_slot(1 - core, p, 1 - b0, 0, 0, 4), :], m_fw.at[t, p, 1])

    tower_backward(qx, wqo, a_q, h_q, u_q, r_q, gp_q)
    pair_start(0, gp_q, pp_q)
    gather_jobs(uall, u0[6:], s_u, m_u)
    pair_send(uall, L0, s_ud, m_ud)
    gather_jobs(uall, u1[:3], s_u, m_u)
    pair_finish(0, gp_q, pp_q, ra_q)

    for k in range(NDEV - 1):
        src = (me + NDEV - 1 - k) % NDEV
        arrived(msgs.at[src], m_msg.at[k])
    total = msgs[0, :, ROWS:MSG]
    for b in range(1, NDEV):
        total = total + msgs[b, :, ROWS:MSG]
    loss_out[...] = jnp.broadcast_to(jnp.sum(total, axis=1, keepdims=True) * (1.0 / TOTAL), (1, 128))

    def dv_block(b, own=False):
        s = dot_nt(vall[me], uall[b])
        p = jnp.exp2(s * LOGIT_SCALE - wide(bcol[...])) * msgs[b, :, 0:ROWS]
        if own:
            p = jnp.where(eye, p - 1.0, p)
        return dot_nn(p.astype(BF16), uall[b])

    def dv_group(blocks):
        total = dacc[...]
        for b in blocks:
            total = total + dv_block(b)
        dacc[...] = total

    def dv_step(g, _):
        @pl.when(g == 1)
        def _():
            gather_jobs(uall, u1[3:], s_u, m_u)
            pair_send(uall, L1, s_ud, m_ud)
            pair_wait(uall, L0, m_ud)

        @pl.when(g == 3)
        def _():
            gather_jobs(uall, u2, s_u, m_u)
            pair_send(uall, L2, s_ud, m_ud)
            pair_wait(uall, L1, m_ud)

        dv_group(group_devs(g))
        return 0

    pair_wait(uall, (0,), m_ud)
    dacc[...] = dv_block(me, True) + dv_block(partner)
    lax.fori_loop(0, 4, dv_step, 0)
    r1_finish(0, pp_q, ra_q, rb_q)
    pair_wait(uall, L2, m_ud)
    dv_group([dev(7), dev_other(7)])
    tower_backward(vx, wvo, a_v, h_v, u_v, r_v, gp_v)
    pair_start(1, gp_v, pp_v)
    r2_finish(0, gq_out, pp_q, rb_q)
    pair_finish(1, gp_v, pp_v, ra_v)
    ag_plane(0, gq_out)
    r1_finish(1, pp_v, ra_v, rb_v)
    ag_axis(0, gq_out)
    r2_finish(1, gv_out, pp_v, rb_v)
    ag_finish(0, gq_out)
    ag_plane(1, gv_out)
    ag_axis(1, gv_out)
    ag_finish(1, gv_out)
    for make in pending:
        rcopy(*make()).wait_send()


def finish(loss, gq, gv, loss_out, gqi, gqo, gvi, gvo, sem):
    copies = []
    for i, (g, gi, go) in enumerate(((gq, gqi, gqo), (gv, gvi, gvo))):
        copies.append(pltpu.make_async_copy(g.at[0:FEAT, :], gi.at[:, 0:EMB], sem.at[i, 0]))
        copies.append(pltpu.make_async_copy(g.at[FEAT:2 * FEAT, :], gi.at[:, EMB:HID], sem.at[i, 1]))
        copies.append(pltpu.make_async_copy(g.at[2 * FEAT:PACK, :], go, sem.at[i, 2]))
    for copy in copies:
        copy.start()
    loss_out[0] = loss[0, 0]
    for copy in copies:
        copy.wait()


def solution(mesh):
    vmem = pl.BlockSpec(memory_space=pltpu.VMEM)
    smem = pl.BlockSpec(memory_space=pltpu.SMEM)
    hbm = pl.BlockSpec(memory_space=pltpu.HBM)
    anym = pl.BlockSpec(memory_space=pl.ANY)
    dma = pltpu.SemaphoreType.DMA
    V = pltpu.VMEM

    def local_step(query_feat, item_feat, log_q, w_query_in, w_query_out, w_item_in, w_item_out):
        shape = jax.ShapeDtypeStruct
        loss, gq, gv = pl.pallas_call(
            kernel,
            out_shape=(shape((1, 128), F32), shape((PACK, EMB), F32), shape((PACK, EMB), F32)),
            in_specs=[hbm] * 7,
            out_specs=(vmem, vmem, vmem),
            scratch_shapes=[
                V((ROWS, FEAT), BF16), V((ROWS, FEAT), BF16),
                V((FEAT, HID), BF16), V((HID, EMB), BF16), V((FEAT, HID), BF16), V((HID, EMB), BF16), dma((7,)),
                V((NDEV, ROWS, EMB), BF16), V((NDEV, ROWS, EMB), BF16),
                V((NDEV, 1, ROWS), F32), V((1, 128), F32),
                V((NDEV, 1, MSG), F32),
                V((ROWS, EMB), F32), V((ROWS, EMB), F32),
                V((ROWS, HID), F32), V((ROWS, HID), F32),
                V((ROWS, HID), BF16), V((ROWS, HID), BF16),
                V((ROWS, EMB), F32), V((ROWS, EMB), F32),
                V((ROWS, EMB), F32), V((ROWS, EMB), F32),
                V((ROWS, EMB), F32), V((ROWS, EMB), F32), V((ROWS, EMB), F32),
                V((PACK, EMB), F32), V((PACK, EMB), F32),
                V((HALF, EMB), F32), V((HALF, EMB), F32),
                V((HALF // 2, EMB), F32), V((HALF // 2, EMB), F32),
                V((3, HALF // 8, EMB), F32), V((3, HALF // 8, EMB), F32),
                dma((15,)), dma((15,)),
                dma((4, 8, 3)), dma((4, 8)), dma((8,)), dma((8,)), dma((8,)), dma((8,)),
                dma((3, 8, 3)), dma((3, 8)), dma((8,)), dma((8,)),
                dma((2,)), dma((2,)), dma((2, 3)), dma((2, 3)), dma((2, 3, 3)), dma((2, 3, 3)),
                dma((2, 3, 3)), dma((2, 3, 3)), dma((2, 3, 4)), dma((2, 3, 4)), dma((2, 3, 2)), dma((2, 3, 2)),
            ],
            compiler_params=pltpu.CompilerParams(collective_id=0, has_side_effects=True,
                                                 vmem_limit_bytes=48 * 1024 * 1024),
            name="step",
        )(*(pltpu.with_memory_space_constraint(x, pltpu.HBM) for x in (
            query_feat, item_feat, log_q.reshape(1, ROWS), w_query_in, w_query_out, w_item_in, w_item_out)))
        return pl.pallas_call(
            finish,
            out_shape=(shape((1,), F32), shape((FEAT, HID), F32), shape((HID, EMB), F32),
                       shape((FEAT, HID), F32), shape((HID, EMB), F32)),
            in_specs=[vmem, vmem, vmem],
            out_specs=(smem, hbm, hbm, hbm, hbm),
            scratch_shapes=[dma((2, 3))],
            compiler_params=pltpu.CompilerParams(vmem_limit_bytes=8 * 1024 * 1024),
            name="finish",
        )(loss, gq, gv)

    return jax.shard_map(local_step, mesh=mesh, in_specs=(P('dp', None), P('dp', None), P('dp'), P(), P(), P(), P()), out_specs=(P(), P(), P(), P(), P()), check_vma=False)
```

```python
import jax
import jax.numpy as jnp
from jax import lax
from jax.experimental import pallas as pl
from jax.experimental.pallas import tpu as pltpu
from jax.sharding import PartitionSpec as P

MESH = pl.DeviceIdType.MESH
TEMPERATURE = 0.05
NORM_EPS = 1e-6
LOG2E = 1.4426950408889634
NDEV = 16
ROWS = 512
FEAT = 512
HID = 256
EMB = 128
PACK = 2 * FEAT + HID
HALF = PACK // 2
SUM_BASE = (0, 192, 384)
SUM_ROWS = (192, 192, 256)
TOTAL = NDEV * ROWS
GRAD_SCALE = 1.0 / (TEMPERATURE * TOTAL)
LOGIT_SCALE = LOG2E / TEMPERATURE
PARTS = ((0, 176), (176, 176), (352, 160))
ORDERS = ((1, 2, 4), (2, 4, 1), (4, 1, 2), (1, 2, 4))
LEVELS = ((1, 2, 4), (6, 5, 3), (7,))
PAIR = ((0,),) + LEVELS
MSG = ROWS + 128
F32 = jnp.float32
BF16 = jnp.bfloat16


def dot_nn(a, b):
    return lax.dot_general(a, b, (((1,), (0,)), ((), ())), preferred_element_type=F32)


def dot_nt(a, b):
    return lax.dot_general(a, b, (((1,), (1,)), ((), ())), preferred_element_type=F32)


def dot_tn(a, b):
    return lax.dot_general(a, b, (((0,), (0,)), ((), ())), preferred_element_type=F32)


def wide(col):
    return jnp.concatenate([col, col, col, col], axis=1)


def kernel(qx_h, vx_h, lq_h, wqi_h, wqo_h, wvi_h, wvo_h,
           loss_out, gq_out, gv_out,
           qx, vx, wqi, wqo, wvi, wvo, s_in,
           uall, vall, lqall, crun, pos_row, msgs, lacc, diag,
           a_q, a_v, h_q, h_v, u_q, u_v, r_q, r_v, invl, bcol, dacc,
           gp_q, gp_v, pp_q, pp_v, ra_q, ra_v, rb_q, rb_v, fin, s_own,
           s_msg, m_msg,
           s_v, m_v, m_vd, m_ld, s_u, m_u, m_ud,
           s_pair, m_pair, s_r1, m_r1, s_r2, m_r2, s_g1, m_g1, s_g2, m_g2, s_fw, m_fw):
    me = lax.axis_index("dp")
    core = me % 2
    bit_x, bit_y, bit_z = (me // 2) % 2, (me // 4) % 2, (me // 8) % 2
    step_x, step_y, step_z = 2 - 4 * bit_x, 4 - 8 * bit_y, 8 - 16 * bit_z
    partner = me + 1 - 2 * core
    chip = me // 2

    def flipped(mask):
        return me + (mask % 2) * step_x + ((mask // 2) % 2) * step_y + (mask // 4) * step_z

    same_core = [flipped(mask) for mask in range(8)]

    def dev(mask):
        return same_core[mask]

    def dev_other(mask):
        return same_core[mask] + partner - me

    def nth_dev(n):
        q, r = (n + 2) // 3, (n + 2) % 3
        base = r * (r + 1) // 2 + 1
        last = q // 5
        mask = (base + q // 3 * (7 - 2 * base)) * ((q + 4) // 5) * (1 - last) + 7 * last
        return flipped(mask) + ((q + 1) % 2 + last * (n - 13)) * (partner - me)

    def rcopy(src, dst, ssem, rsem, to):
        return pltpu.make_async_remote_copy(src_ref=src, dst_ref=dst, send_sem=ssem, recv_sem=rsem,
                                            device_id=(to,), device_id_type=MESH)

    def send(src, dst, ssem, rsem, to):
        rcopy(src, dst, ssem, rsem, to).start()

    def sent(like, ssem):
        rcopy(like, like, ssem, ssem, partner).wait_send()

    def arrived(ref, rsem):
        rcopy(ref, ref, rsem, rsem, partner).wait_recv()

    others = [(me + k) % NDEV for k in range(1, NDEV)]

    loads = [pltpu.make_async_copy(src, dst, s_in.at[i]) for i, (src, dst) in enumerate((
        (vx_h, vx), (wvi_h, wvi), (wvo_h, wvo), (lq_h, lqall.at[me]), (qx_h, qx), (wqi_h, wqi), (wqo_h, wqo)))]
    for load in loads:
        load.start()
    barrier = pltpu.get_barrier_semaphore()
    for to in (partner, dev(1), dev(2), dev(4)):
        pl.semaphore_signal(barrier, inc=1, device_id=(to,), device_id_type=MESH)

    def tower_forward(x, w_in, w_out, a_ref, h_ref, u_ref, r_ref, all_ref):
        a = dot_nn(x[...], w_in[...])
        a_ref[...] = a
        h = jnp.maximum(a, 0.0).astype(BF16)
        h_ref[...] = h
        e = dot_nn(h, w_out[...])
        r = lax.rsqrt(jnp.sum(e * e, axis=-1, keepdims=True) + NORM_EPS)
        u = e * r
        u_ref[...] = u
        r_ref[...] = jnp.broadcast_to(r, (ROWS, EMB))
        all_ref[me] = u.astype(BF16)

    for load in loads[:4]:
        load.wait()
    tower_forward(vx, wvi, wvo, a_v, h_v, u_v, r_v, vall)
    pl.semaphore_wait(barrier, 4)

    def part_ref(ref, src, p):
        if p == 3:
            return lqall.at[src]
        return ref.at[src, pl.ds(PARTS[p][0], PARTS[p][1]), :]

    def send_part(ref, p, m, t, ss, ms):
        d = ORDERS[p][t]
        src = part_ref(ref, dev(m), p)
        send(src, src, ss.at[p // 3], ms.at[p % 3, m + d], dev(d))

    def gather_own(ref, ts, ps, ss, ms):
        for t in ts:
            for p in ps:
                send_part(ref, p, 0, t, ss, ms)

    def level_jobs(level, ps):
        jobs = []
        for p in ps:
            for m in LEVELS[level]:
                top = max(t for t in range(3) if ORDERS[p][t] & m)
                jobs.append((top, p, m))
        return sorted(jobs)

    def gather_jobs(ref, jobs, ss, ms):
        for top, p, m in jobs:
            src = dev(m)
            if p == 0 and ref is vall:
                arrived(ref.at[src, 0:PARTS[0][1] + 8, :], ms.at[0, m])
                for t in range(top + 1, 3):
                    send_part(ref, 3, m, t, ss, ms)
            else:
                arrived(part_ref(ref, src, p), ms.at[p, m])
            for t in range(top + 1, 3):
                send_part(ref, p, m, t, ss, ms)

    def pair_send(ref, level, sd, md):
        for m in PAIR[level]:
            send(ref.at[dev(m)], ref.at[dev(m)], sd, md.at[level], partner)

    def pair_wait(ref, level, md):
        arrived(ref.at[0:len(PAIR[level])], md.at[level])

    VP, UP = (3, 0, 1, 2), (0, 1, 2)
    pair_send(lqall, 0, s_v.at[3], m_ld)
    pair_send(vall, 0, s_v.at[2], m_vd)
    gather_own(vall, (0, 1, 2), VP, s_v, m_v)

    for load in loads[4:]:
        load.wait()
    tower_forward(qx, wqi, wqo, a_q, h_q, u_q, r_q, uall)
    pair_send(uall, 0, s_u.at[1], m_ud)

    eye = (lax.broadcasted_iota(jnp.int32, (ROWS, ROWS), 0)
           == lax.broadcasted_iota(jnp.int32, (ROWS, ROWS), 1))

    def block_shift(b):
        return jnp.max(-lqall[b], axis=1, keepdims=True)

    def exp_block(b, c):
        s = dot_nt(uall[me], vall[b])
        return jnp.exp2(s * LOGIT_SCALE - (lqall[b] + c) * LOG2E)

    def lane_sum(e):
        return e[:, 0:128] + e[:, 128:256] + (e[:, 256:384] + e[:, 384:512])

    def exp_group(blocks):
        c_old = crun[...]
        c = c_old
        for b in blocks:
            c = jnp.maximum(c, block_shift(b))
        crun[...] = c
        scale = jnp.exp2((c_old - c) * LOG2E)
        l_new, d_new = lacc[...] * scale, dacc[...] * scale
        for b in blocks:
            e = exp_block(b, c[:, 0:1])
            l_new = l_new + lane_sum(e)
            d_new = d_new + dot_nn(e.astype(BF16), vall[b])
        lacc[...], dacc[...] = l_new, d_new

    c_own = block_shift(me)
    crun[...] = jnp.broadcast_to(c_own, (1, 128))
    e_own = exp_block(me, c_own)
    lacc[...] = lane_sum(e_own)
    diag[...] = jnp.broadcast_to(jnp.sum(jnp.where(eye, e_own, 0.0), axis=1, keepdims=True), (ROWS, EMB))
    dacc[...] = dot_nn(jnp.where(eye, 0.0, e_own).astype(BF16), vall[me])
    pos_row[...] = jnp.sum((uall[me].astype(F32) * vall[me].astype(F32)).T, axis=0, keepdims=True) * (1.0 / TEMPERATURE)

    v0, v1, v2 = (level_jobs(k, UP) for k in range(3))
    u0, u1, u2 = (level_jobs(k, UP) for k in range(3))

    def exp_step(g, _):
        @pl.when(g == 0)
        def _():
            gather_jobs(vall, v0, s_v, m_v)
            pair_send(lqall, 1, s_v.at[3], m_ld)
            pair_send(vall, 1, s_v.at[2], m_vd)
            pair_wait(lqall, 0, m_ld)
            pair_wait(vall, 0, m_vd)

        @pl.when(g == 1)
        def _():
            gather_jobs(vall, v1[:3], s_v, m_v)
            gather_own(uall, (0, 1, 2), UP, s_u, m_u)
            pair_wait(lqall, 1, m_ld)
            pair_wait(vall, 1, m_vd)

        @pl.when(g == 2)
        def _():
            gather_jobs(vall, v1[3:], s_v, m_v)
            pair_send(lqall, 2, s_v.at[3], m_ld)
            pair_send(vall, 2, s_v.at[2], m_vd)

        @pl.when(g == 3)
        def _():
            gather_jobs(vall, v2, s_v, m_v)
            pair_send(lqall, 3, s_v.at[3], m_ld)
            pair_send(vall, 3, s_v.at[2], m_vd)
            pair_wait(lqall, 2, m_ld)
            pair_wait(vall, 2, m_vd)

        @pl.when(g == 4)
        def _():
            gather_jobs(uall, u0[:3], s_u, m_u)
            pair_wait(lqall, 3, m_ld)
            pair_wait(vall, 3, m_vd)

        exp_group([nth_dev(3 * g + j) for j in range(3)])
        return 0

    lax.fori_loop(0, 5, exp_step, 0)

    acc = lacc[...]
    shift = crun[0:1, 0:1]
    lq_own = lqall[me]
    l_row = jnp.sum(acc.T, axis=0, keepdims=True)
    loss_row = jnp.log(l_row) + ((shift + lq_own) - pos_row[...])
    loss_part = loss_row[:, 0:128] + loss_row[:, 128:256] + (loss_row[:, 256:384] + loss_row[:, 384:512])
    msgs[me, :, 0:ROWS] = 1.0 / l_row
    msgs[me, :, ROWS:MSG] = loss_part
    for k in range(NDEV - 1):
        send(msgs.at[me], msgs.at[me], s_msg.at[0], m_msg.at[0], others[k])
    invl[...] = jnp.broadcast_to(1.0 / jnp.sum(acc, axis=1, keepdims=True), (ROWS, EMB))
    bcol[...] = jnp.broadcast_to((lq_own + shift) * LOG2E, (EMB, ROWS)).T

    p_own = diag[...] * jnp.exp2((c_own - crun[...]) * LOG2E) * invl[...]
    dacc[...] = dacc[...] * invl[...] + (p_own - 1.0).astype(BF16).astype(F32) * vall[me].astype(F32)
    gather_jobs(uall, u0[3:6], s_u, m_u)

    def tower_backward(x, w_out, a_ref, h_ref, u_ref, r_ref, g):
        du = dacc[...] * GRAD_SCALE
        u = u_ref[...]
        de = (r_ref[...] * (du - u * jnp.sum(u * du, axis=-1, keepdims=True))).astype(BF16)
        g[2 * FEAT:PACK, :] = dot_tn(h_ref[...], de)
        dh = dot_nt(de, w_out[...])
        da = jnp.where(a_ref[...] > 0, dh, 0.0).astype(BF16)
        gi = dot_tn(x[...], da)
        g[0:FEAT, :] = gi[:, 0:EMB]
        g[FEAT:2 * FEAT, :] = gi[:, EMB:HID]

    bit = {1: bit_x, 2: bit_y, 4: bit_z}
    PLANE = ((0, 1), (1, 0), (1, 1))

    def rows(base, size):
        return pl.ds(pl.multiple_of(base, 8), size)

    def slot(p, b0, b1, b2, count):
        eighth = SUM_ROWS[p] // 8
        return rows(SUM_BASE[p] + (b0 * 4 + b1 * 2 + b2) * eighth, count * eighth)

    def half(c):
        return rows(c * HALF, HALF)

    def out_slot(c, p, b0, b1, b2, count):
        eighth = SUM_ROWS[p] // 8
        return rows(c * HALF + SUM_BASE[p] + (b0 * 4 + b1 * 2 + b2) * eighth, count * eighth)

    def bits(p, f1=0, f2=0):
        d0, d1, d2 = ORDERS[p]
        b1 = bit[d1] if not f1 else 1 - bit[d1]
        b2 = bit[d2] if not f2 else 1 - bit[d2]
        return bit[d0], b1, b2

    def plane_dev(p, k):
        return dev(PLANE[k][0] * ORDERS[p][1] + PLANE[k][1] * ORDERS[p][2])

    def like_shard(out, p):
        return out.at[0:SUM_ROWS[p] // 8, :]

    def plane_shard(out, p, k):
        return out.at[out_slot(core, p, *bits(p, *PLANE[k]), 1), :]

    def axis_half(out, p, far):
        b0 = bits(p)[0]
        return out.at[out_slot(core, p, 1 - b0 if far else b0, 0, 0, 4), :]

    def pair_start(t, g, pp):
        send(g.at[half(1 - core), :], pp, s_pair.at[t], m_pair.at[t], partner)

    def pair_finish(t, g, pp, ra):
        arrived(pp, m_pair.at[t])
        pp[...] = pp[...] + g[half(core), :]
        for p in range(3):
            part = ra.at[pl.ds(SUM_BASE[p] // 2, SUM_ROWS[p] // 2), :]
            send(pp.at[slot(p, 1 - bits(p)[0], 0, 0, 4), :], part, s_r1.at[t], m_r1.at[t, p], dev(ORDERS[p][0]))

    def r1_finish(t, pp, ra, rb):
        for p in range(3):
            part = pl.ds(SUM_BASE[p] // 2, SUM_ROWS[p] // 2)
            arrived(ra.at[part, :], m_r1.at[t, p])
            b0, _, _ = bits(p)
            mine = slot(p, b0, 0, 0, 4)
            pp[mine, :] = pp[mine, :] + ra[part, :]
        for k in (2, 0, 1):
            for p in range(3):
                part = rb.at[k, pl.ds(SUM_BASE[p] // 8, SUM_ROWS[p] // 8), :]
                send(pp.at[slot(p, *bits(p, *PLANE[k]), 1), :], part, s_r2.at[t], m_r2.at[t, p], plane_dev(p, k))

    def r2_finish(t, out, pp, rb):
        for p in range(3):
            part = pl.ds(SUM_BASE[p] // 8, SUM_ROWS[p] // 8)
            total = pp[slot(p, *bits(p), 1), :]
            arrived(rb.at[:, part, :], m_r2.at[t, p])
            for k in range(3):
                total = total + rb[k, part, :]
            own = fin.at[t, pl.ds(SUM_BASE[p] // 8, SUM_ROWS[p] // 8), :]
            fin[t, SUM_BASE[p] // 8:(SUM_BASE[p] + SUM_ROWS[p]) // 8, :] = total
            place = out.at[out_slot(core, p, *bits(p), 1), :]
            keep = pltpu.make_async_copy(own, place, s_own.at[t, p])
            keep.start()
            for k in (2, 0, 1):
                send(own, place, s_g1.at[t], m_g1.at[t, p, k], plane_dev(p, k))
            send(own, place, s_g2.at[t], m_g2.at[t, p], dev(ORDERS[p][0]))

    def ag_plane(t, out):
        for k in range(3):
            for p in range(3):
                ref = plane_shard(out, p, k)
                arrived(ref, m_g1.at[t, p, k])
                send(ref, ref, s_g2.at[t], m_g2.at[t, p], dev(ORDERS[p][0]))
        for p in range(3):
            pltpu.make_async_copy(like_shard(out, p), like_shard(out, p), s_own.at[t, p]).wait()
            ref = axis_half(out, p, 0)
            send(ref, ref, s_fw.at[t], m_fw.at[t], partner)

    def ag_axis(t, out):
        for p in range(3):
            ref = axis_half(out, p, 1)
            arrived(ref, m_g2.at[t, p])
            send(ref, ref, s_fw.at[t], m_fw.at[t], partner)

    def ag_finish(t, out):
        arrived(out.at[0:HALF, :], m_fw.at[t])

    def sums_sent(t, out, pp, ra, rb):
        sent(pp, s_pair.at[t])
        sent(ra, s_r1.at[t])
        sent(rb, s_r2.at[t])
        sent(rb, s_g1.at[t])
        sent(ra, s_g2.at[t])
        sent(pp, s_fw.at[t])

    tower_backward(qx, wqo, a_q, h_q, u_q, r_q, gp_q)
    pair_start(0, gp_q, pp_q)
    gather_jobs(uall, u0[6:], s_u, m_u)
    pair_send(uall, 1, s_u.at[1], m_ud)
    gather_jobs(uall, u1[:3], s_u, m_u)
    pair_finish(0, gp_q, pp_q, ra_q)

    arrived(msgs.at[0:NDEV - 1], m_msg.at[0])
    total = msgs[0, :, ROWS:MSG]
    for b in range(1, NDEV):
        total = total + msgs[b, :, ROWS:MSG]
    loss_out[...] = jnp.broadcast_to(jnp.sum(total, axis=1, keepdims=True) * (1.0 / TOTAL), (1, 128))

    def dv_block(b, own=False):
        s = dot_nt(vall[me], uall[b])
        p = jnp.exp2(s * LOGIT_SCALE - wide(bcol[...])) * msgs[b, :, 0:ROWS]
        if own:
            p = jnp.where(eye, p - 1.0, p)
        return dot_nn(p.astype(BF16), uall[b])

    def dv_group(blocks):
        total = dacc[...]
        for b in blocks:
            total = total + dv_block(b)
        dacc[...] = total

    def dv_step(g, _):
        @pl.when(g == 1)
        def _():
            gather_jobs(uall, u1[3:], s_u, m_u)
            pair_send(uall, 2, s_u.at[1], m_ud)
            pair_wait(uall, 1, m_ud)

        @pl.when(g == 2)
        def _():
            r1_finish(0, pp_q, ra_q, rb_q)

        @pl.when(g == 3)
        def _():
            gather_jobs(uall, u2, s_u, m_u)
            pair_send(uall, 3, s_u.at[1], m_ud)
            pair_wait(uall, 2, m_ud)

        @pl.when(g == 4)
        def _():
            pair_wait(uall, 3, m_ud)
            r2_finish(0, gq_out, pp_q, rb_q)

        dv_group([nth_dev(3 * g + j) for j in range(3)])
        return 0

    pair_wait(uall, 0, m_ud)
    dacc[...] = dv_block(me, True)
    lax.fori_loop(0, 5, dv_step, 0)
    tower_backward(vx, wvo, a_v, h_v, u_v, r_v, gp_v)
    pair_start(1, gp_v, pp_v)
    sent(vall.at[0:7], s_v.at[0])
    sent(lqall.at[0:7], s_v.at[1])
    sent(vall.at[0:8], s_v.at[2])
    sent(lqall.at[0:8], s_v.at[3])
    sent(uall.at[0:7], s_u.at[0])
    sent(uall.at[0:8], s_u.at[1])
    sent(msgs.at[0:NDEV - 1], s_msg.at[0])
    pair_finish(1, gp_v, pp_v, ra_v)
    ag_plane(0, gq_out)
    r1_finish(1, pp_v, ra_v, rb_v)
    ag_axis(0, gq_out)
    r2_finish(1, gv_out, pp_v, rb_v)
    ag_finish(0, gq_out)
    sums_sent(0, gq_out, pp_q, ra_q, rb_q)
    ag_plane(1, gv_out)
    ag_axis(1, gv_out)
    ag_finish(1, gv_out)
    sums_sent(1, gv_out, pp_v, ra_v, rb_v)


def finish(loss, gq, gv, loss_out, gqi, gqo, gvi, gvo, sem):
    copies = []
    for i, (g, gi, go) in enumerate(((gq, gqi, gqo), (gv, gvi, gvo))):
        copies.append(pltpu.make_async_copy(g.at[0:FEAT, :], gi.at[:, 0:EMB], sem.at[i, 0]))
        copies.append(pltpu.make_async_copy(g.at[FEAT:2 * FEAT, :], gi.at[:, EMB:HID], sem.at[i, 1]))
        copies.append(pltpu.make_async_copy(g.at[2 * FEAT:PACK, :], go, sem.at[i, 2]))
    for copy in copies:
        copy.start()
    loss_out[0] = loss[0, 0]
    for copy in copies:
        copy.wait()


def solution(mesh):
    vmem = pl.BlockSpec(memory_space=pltpu.VMEM)
    smem = pl.BlockSpec(memory_space=pltpu.SMEM)
    hbm = pl.BlockSpec(memory_space=pltpu.HBM)
    anym = pl.BlockSpec(memory_space=pl.ANY)
    dma = pltpu.SemaphoreType.DMA
    V = pltpu.VMEM

    def local_step(query_feat, item_feat, log_q, w_query_in, w_query_out, w_item_in, w_item_out):
        shape = jax.ShapeDtypeStruct
        loss, gq, gv = pl.pallas_call(
            kernel,
            out_shape=(shape((1, 128), F32), shape((PACK, EMB), F32), shape((PACK, EMB), F32)),
            in_specs=[hbm] * 7,
            out_specs=(vmem, anym, anym),
            scratch_shapes=[
                V((ROWS, FEAT), BF16), V((ROWS, FEAT), BF16),
                V((FEAT, HID), BF16), V((HID, EMB), BF16), V((FEAT, HID), BF16), V((HID, EMB), BF16), dma((7,)),
                V((NDEV, ROWS, EMB), BF16), V((NDEV, ROWS, EMB), BF16),
                V((NDEV, 1, ROWS), F32), V((1, 128), F32), V((1, ROWS), F32),
                V((NDEV, 1, MSG), F32),
                V((ROWS, EMB), F32), V((ROWS, EMB), F32),
                V((ROWS, HID), F32), V((ROWS, HID), F32),
                V((ROWS, HID), BF16), V((ROWS, HID), BF16),
                V((ROWS, EMB), F32), V((ROWS, EMB), F32),
                V((ROWS, EMB), F32), V((ROWS, EMB), F32),
                V((ROWS, EMB), F32), V((ROWS, EMB), F32), V((ROWS, EMB), F32),
                V((PACK, EMB), F32), V((PACK, EMB), F32),
                V((HALF, EMB), F32), V((HALF, EMB), F32),
                V((HALF // 2, EMB), F32), V((HALF // 2, EMB), F32),
                V((3, HALF // 8, EMB), F32), V((3, HALF // 8, EMB), F32), V((2, HALF // 8, EMB), F32), dma((2, 3)),
                dma((1,)), dma((1,)),
                dma((4,)), dma((3, 8)), dma((4,)), dma((4,)), dma((2,)), dma((3, 8)), dma((4,)),
                dma((2,)), dma((2,)), dma((2,)), dma((2, 3)), dma((2,)), dma((2, 3)),
                dma((2,)), dma((2, 3, 3)), dma((2,)), dma((2, 3)), dma((2,)), dma((2,)),
            ],
            compiler_params=pltpu.CompilerParams(collective_id=0, has_side_effects=True,
                                                 vmem_limit_bytes=48 * 1024 * 1024),
            name="step",
        )(*(pltpu.with_memory_space_constraint(x, pltpu.HBM) for x in (
            query_feat, item_feat, log_q.reshape(1, ROWS), w_query_in, w_query_out, w_item_in, w_item_out)))
        return pl.pallas_call(
            finish,
            out_shape=(shape((1,), F32), shape((FEAT, HID), F32), shape((HID, EMB), F32),
                       shape((FEAT, HID), F32), shape((HID, EMB), F32)),
            in_specs=[vmem, anym, anym],
            out_specs=(smem, hbm, hbm, hbm, hbm),
            scratch_shapes=[dma((2, 3))],
            compiler_params=pltpu.CompilerParams(vmem_limit_bytes=8 * 1024 * 1024),
            name="finish",
        )(loss, gq, gv)

    return jax.shard_map(local_step, mesh=mesh, in_specs=(P('dp', None), P('dp', None), P('dp'), P(), P(), P(), P()), out_specs=(P(), P(), P(), P(), P()), check_vma=False)
```

```python
import jax
import jax.numpy as jnp
from jax import lax
from jax.experimental import pallas as pl
from jax.experimental.pallas import tpu as pltpu
from jax.sharding import PartitionSpec as P

MESH = pl.DeviceIdType.MESH
TEMPERATURE = 0.05
NORM_EPS = 1e-6
LOG2E = 1.4426950408889634
NDEV = 16
ROWS = 512
FEAT = 512
HID = 256
EMB = 128
PACK = 2 * FEAT + HID
HALF = PACK // 2
SUM_BASE = (0, 192, 384)
SUM_ROWS = (192, 192, 256)
TOTAL = NDEV * ROWS
GRAD_SCALE = 1.0 / (TEMPERATURE * TOTAL)
LOGIT_SCALE = LOG2E / TEMPERATURE
PARTS = ((0, 176), (176, 176), (352, 160))
ORDERS = ((1, 2, 4), (2, 4, 1), (4, 1, 2), (1, 2, 4))
LEVELS = ((1, 2, 4), (6, 5, 3), (7,))
PAIR = ((0,),) + LEVELS
SLOT = {(0, 0): 0, (0, 1): 1, (0, 2): 2, (1, 1): 3, (1, 2): 4, (2, 2): 5}
MSG = ROWS + 128
F32 = jnp.float32
BF16 = jnp.bfloat16


def dot_nn(a, b):
    return lax.dot_general(a, b, (((1,), (0,)), ((), ())), preferred_element_type=F32)


def dot_nt(a, b):
    return lax.dot_general(a, b, (((1,), (1,)), ((), ())), preferred_element_type=F32)


def dot_tn(a, b):
    return lax.dot_general(a, b, (((0,), (0,)), ((), ())), preferred_element_type=F32)


def wide(col):
    return jnp.concatenate([col, col, col, col], axis=1)


def kernel(qx_h, vx_h, lq_h, wqi_h, wqo_h, wvi_h, wvo_h,
           loss_out, gq_out, gv_out,
           qx, vx, wqi, wqo, wvi, wvo, s_in,
           uall, vall, lqall, crun, pos_row, msgs, lacc, diag,
           a_q, a_v, h_q, h_v, u_q, u_v, r_q, r_v, invl, bcol, dacc,
           gp_q, gp_v, pp_q, pp_v, ra_q, ra_v, rb_q, rb_v, fin, s_own,
           s_msg, m_msg,
           s_v, m_v, m_l, m_vd, m_ld, s_u, m_u, m_ud,
           s_pair, m_pair, s_r1, m_r1, s_r2, m_r2, s_g1, m_g1, s_g2, m_g2, s_fw, m_fw):
    me = lax.axis_index("dp")
    core = me % 2
    bit_x, bit_y, bit_z = (me // 2) % 2, (me // 4) % 2, (me // 8) % 2
    step_x, step_y, step_z = 2 - 4 * bit_x, 4 - 8 * bit_y, 8 - 16 * bit_z
    partner = me + 1 - 2 * core
    chip = me // 2

    def flipped(mask):
        return me + (mask % 2) * step_x + ((mask // 2) % 2) * step_y + (mask // 4) * step_z

    same_core = [flipped(mask) for mask in range(8)]

    def dev(mask):
        return same_core[mask]

    def dev_other(mask):
        return same_core[mask] + partner - me

    def nth_dev(n):
        q, r = (n + 2) // 3, (n + 2) % 3
        base = r * (r + 1) // 2 + 1
        last = q // 5
        mask = (base + q // 3 * (7 - 2 * base)) * ((q + 4) // 5) * (1 - last) + 7 * last
        return flipped(mask) + ((q + 1) % 2 + last * (n - 13)) * (partner - me)

    def rcopy(src, dst, ssem, rsem, to):
        return pltpu.make_async_remote_copy(src_ref=src, dst_ref=dst, send_sem=ssem, recv_sem=rsem,
                                            device_id=(to,), device_id_type=MESH)

    def send(src, dst, ssem, rsem, to):
        rcopy(src, dst, ssem, rsem, to).start()

    def sent(like, ssem):
        rcopy(like, like, ssem, ssem, partner).wait_send()

    def arrived(ref, rsem):
        rcopy(ref, ref, rsem, rsem, partner).wait_recv()

    others = [(me + k) % NDEV for k in range(1, NDEV)]

    loads = [pltpu.make_async_copy(src, dst, s_in.at[i]) for i, (src, dst) in enumerate((
        (vx_h, vx), (wvi_h, wvi), (wvo_h, wvo), (lq_h, lqall.at[me]), (qx_h, qx), (wqi_h, wqi), (wqo_h, wqo)))]
    for load in loads:
        load.start()
    barrier = pltpu.get_barrier_semaphore()
    for to in (partner, dev(1), dev(2), dev(4)):
        pl.semaphore_signal(barrier, inc=1, device_id=(to,), device_id_type=MESH)

    def tower_forward(x, w_in, w_out, a_ref, h_ref, u_ref, r_ref, all_ref):
        a = dot_nn(x[...], w_in[...])
        a_ref[...] = a
        h = jnp.maximum(a, 0.0).astype(BF16)
        h_ref[...] = h
        e = dot_nn(h, w_out[...])
        r = lax.rsqrt(jnp.sum(e * e, axis=-1, keepdims=True) + NORM_EPS)
        u = e * r
        u_ref[...] = u
        r_ref[...] = jnp.broadcast_to(r, (ROWS, EMB))
        all_ref[me] = u.astype(BF16)

    for load in loads[:4]:
        load.wait()
    tower_forward(vx, wvi, wvo, a_v, h_v, u_v, r_v, vall)
    pl.semaphore_wait(barrier, 4)

    def part_ref(ref, src, p):
        if p == 3:
            return lqall.at[src]
        return ref.at[src, pl.ds(PARTS[p][0], PARTS[p][1]), :]

    def send_part(ref, p, m, t, ss, ms):
        d = ORDERS[p][t]
        src = part_ref(ref, dev(m), p)
        to = m + d
        rsem = ms.at[to] if p == 3 else ms.at[SLOT[bin(to).count("1") - 1, top_turn(p, to)]]
        send(src, src, ss.at[p // 3], rsem, dev(d))

    def gather_own(ref, ts, ss, ms):
        for t in ts:
            for p in range(3):
                send_part(ref, p, 0, t, ss, ms)

    def top_turn(p, m):
        return max(t for t in range(3) if ORDERS[p][t] & m)

    def gather_jobs(ref, level, t, ss, ms, ml=None):
        jobs = [(p, m) for p in range(3) for m in LEVELS[level] if top_turn(p, m) == t]
        arrived(ref.at[0:len(jobs) // 3] if len(jobs) > 3 else ref.at[0], ms.at[SLOT[level, t]])
        if ml is not None:
            for m in sorted({m for m in LEVELS[level] if top_turn(3, m) == t}):
                arrived(lqall.at[dev(m)], ml.at[m])
                for tt in range(t + 1, 3):
                    send_part(lqall, 3, m, tt, ss, ml)
        for p, m in jobs:
            for tt in range(t + 1, 3):
                send_part(ref, p, m, tt, ss, ms)

    def pair_send(ref, level, sd, md):
        for m in PAIR[level]:
            send(ref.at[dev(m)], ref.at[dev(m)], sd, md.at[level], partner)

    def pair_wait(ref, level, md):
        arrived(ref.at[0:len(PAIR[level])], md.at[level])

    pair_send(lqall, 0, s_v.at[3], m_ld)
    pair_send(vall, 0, s_v.at[2], m_vd)
    for t in range(3):
        send_part(lqall, 3, 0, t, s_v, m_l)
    gather_own(vall, (0, 1, 2), s_v, m_v)

    for load in loads[4:]:
        load.wait()
    tower_forward(qx, wqi, wqo, a_q, h_q, u_q, r_q, uall)
    pair_send(uall, 0, s_u.at[1], m_ud)

    eye = (lax.broadcasted_iota(jnp.int32, (ROWS, ROWS), 0)
           == lax.broadcasted_iota(jnp.int32, (ROWS, ROWS), 1))

    def block_shift(b):
        return jnp.max(-lqall[b], axis=1, keepdims=True)

    def exp_block(b, c):
        s = dot_nt(uall[me], vall[b])
        return jnp.exp2(s * LOGIT_SCALE - (lqall[b] + c) * LOG2E)

    def lane_sum(e):
        return e[:, 0:128] + e[:, 128:256] + (e[:, 256:384] + e[:, 384:512])

    def exp_group(blocks):
        c_old = crun[...]
        c = c_old
        for b in blocks:
            c = jnp.maximum(c, block_shift(b))
        crun[...] = c
        scale = jnp.exp2((c_old - c) * LOG2E)
        l_new, d_new = lacc[...] * scale, dacc[...] * scale
        for b in blocks:
            e = exp_block(b, c[:, 0:1])
            l_new = l_new + lane_sum(e)
            d_new = d_new + dot_nn(e.astype(BF16), vall[b])
        lacc[...], dacc[...] = l_new, d_new

    c_own = block_shift(me)
    crun[...] = jnp.broadcast_to(c_own, (1, 128))
    e_own = exp_block(me, c_own)
    lacc[...] = lane_sum(e_own)
    diag[...] = jnp.broadcast_to(jnp.sum(jnp.where(eye, e_own, 0.0), axis=1, keepdims=True), (ROWS, EMB))
    dacc[...] = dot_nn(jnp.where(eye, 0.0, e_own).astype(BF16), vall[me])
    pos_row[...] = jnp.sum((uall[me].astype(F32) * vall[me].astype(F32)).T, axis=0, keepdims=True) * (1.0 / TEMPERATURE)

    def exp_step(g, _):
        @pl.when(g == 0)
        def _():
            for t in range(3):
                gather_jobs(vall, 0, t, s_v, m_v, m_l)
            pair_send(lqall, 1, s_v.at[3], m_ld)
            pair_send(vall, 1, s_v.at[2], m_vd)
            pair_wait(lqall, 0, m_ld)
            pair_wait(vall, 0, m_vd)

        @pl.when(g == 1)
        def _():
            gather_jobs(vall, 1, 1, s_v, m_v, m_l)
            gather_own(uall, (0, 1, 2), s_u, m_u)
            pair_wait(lqall, 1, m_ld)
            pair_wait(vall, 1, m_vd)

        @pl.when(g == 2)
        def _():
            gather_jobs(vall, 1, 2, s_v, m_v, m_l)
            pair_send(lqall, 2, s_v.at[3], m_ld)
            pair_send(vall, 2, s_v.at[2], m_vd)

        @pl.when(g == 3)
        def _():
            gather_jobs(vall, 2, 2, s_v, m_v, m_l)
            pair_send(lqall, 3, s_v.at[3], m_ld)
            pair_send(vall, 3, s_v.at[2], m_vd)
            pair_wait(lqall, 2, m_ld)
            pair_wait(vall, 2, m_vd)

        @pl.when(g == 4)
        def _():
            gather_jobs(uall, 0, 0, s_u, m_u)
            pair_wait(lqall, 3, m_ld)
            pair_wait(vall, 3, m_vd)

        exp_group([nth_dev(3 * g + j) for j in range(3)])
        return 0

    lax.fori_loop(0, 5, exp_step, 0)

    acc = lacc[...]
    shift = crun[0:1, 0:1]
    lq_own = lqall[me]
    l_row = jnp.sum(acc.T, axis=0, keepdims=True)
    loss_row = jnp.log(l_row) + ((shift + lq_own) - pos_row[...])
    loss_part = loss_row[:, 0:128] + loss_row[:, 128:256] + (loss_row[:, 256:384] + loss_row[:, 384:512])
    msgs[me, :, 0:ROWS] = 1.0 / l_row
    msgs[me, :, ROWS:MSG] = loss_part
    for k in range(NDEV - 1):
        send(msgs.at[me], msgs.at[me], s_msg.at[0], m_msg.at[0], others[k])
    invl[...] = jnp.broadcast_to(1.0 / jnp.sum(acc, axis=1, keepdims=True), (ROWS, EMB))
    bcol[...] = jnp.broadcast_to((lq_own + shift) * LOG2E, (EMB, ROWS)).T

    p_own = diag[...] * jnp.exp2((c_own - crun[...]) * LOG2E) * invl[...]
    dacc[...] = dacc[...] * invl[...] + (p_own - 1.0).astype(BF16).astype(F32) * vall[me].astype(F32)
    gather_jobs(uall, 0, 1, s_u, m_u)

    def tower_backward(x, w_out, a_ref, h_ref, u_ref, r_ref, g):
        du = dacc[...] * GRAD_SCALE
        u = u_ref[...]
        de = (r_ref[...] * (du - u * jnp.sum(u * du, axis=-1, keepdims=True))).astype(BF16)
        g[2 * FEAT:PACK, :] = dot_tn(h_ref[...], de)
        dh = dot_nt(de, w_out[...])
        da = jnp.where(a_ref[...] > 0, dh, 0.0).astype(BF16)
        gi = dot_tn(x[...], da)
        g[0:FEAT, :] = gi[:, 0:EMB]
        g[FEAT:2 * FEAT, :] = gi[:, EMB:HID]

    bit = {1: bit_x, 2: bit_y, 4: bit_z}
    PLANE = ((0, 1), (1, 0), (1, 1))

    def rows(base, size):
        return pl.ds(pl.multiple_of(base, 8), size)

    def slot(p, b0, b1, b2, count):
        eighth = SUM_ROWS[p] // 8
        return rows(SUM_BASE[p] + (b0 * 4 + b1 * 2 + b2) * eighth, count * eighth)

    def half(c):
        return rows(c * HALF, HALF)

    def out_slot(c, p, b0, b1, b2, count):
        eighth = SUM_ROWS[p] // 8
        return rows(c * HALF + SUM_BASE[p] + (b0 * 4 + b1 * 2 + b2) * eighth, count * eighth)

    def bits(p, f1=0, f2=0):
        d0, d1, d2 = ORDERS[p]
        b1 = bit[d1] if not f1 else 1 - bit[d1]
        b2 = bit[d2] if not f2 else 1 - bit[d2]
        return bit[d0], b1, b2

    def plane_dev(p, k):
        return dev(PLANE[k][0] * ORDERS[p][1] + PLANE[k][1] * ORDERS[p][2])

    def plane_shard(out, p, k):
        return out.at[out_slot(core, p, *bits(p, *PLANE[k]), 1), :]

    def axis_half(out, p, far):
        b0 = bits(p)[0]
        return out.at[out_slot(core, p, 1 - b0 if far else b0, 0, 0, 4), :]

    def pair_start(t, g, pp):
        send(g.at[half(1 - core), :], pp, s_pair.at[t], m_pair.at[t], partner)

    def pair_finish(t, g, pp, ra):
        arrived(pp, m_pair.at[t])
        pp[...] = pp[...] + g[half(core), :]
        for p in range(3):
            part = ra.at[pl.ds(SUM_BASE[p] // 2, SUM_ROWS[p] // 2), :]
            send(pp.at[slot(p, 1 - bits(p)[0], 0, 0, 4), :], part, s_r1.at[t], m_r1.at[t], dev(ORDERS[p][0]))

    def r1_finish(t, pp, ra, rb):
        arrived(ra, m_r1.at[t])
        for p in range(3):
            part = pl.ds(SUM_BASE[p] // 2, SUM_ROWS[p] // 2)
            b0, _, _ = bits(p)
            mine = slot(p, b0, 0, 0, 4)
            pp[mine, :] = pp[mine, :] + ra[part, :]
        for k in (2, 0, 1):
            for p in range(3):
                part = rb.at[k, pl.ds(SUM_BASE[p] // 8, SUM_ROWS[p] // 8), :]
                send(pp.at[slot(p, *bits(p, *PLANE[k]), 1), :], part, s_r2.at[t], m_r2.at[t], plane_dev(p, k))

    def r2_finish(t, out, pp, rb):
        arrived(rb, m_r2.at[t])
        for p in range(3):
            part = pl.ds(SUM_BASE[p] // 8, SUM_ROWS[p] // 8)
            total = pp[slot(p, *bits(p), 1), :]
            for k in range(3):
                total = total + rb[k, part, :]
            own = fin.at[t, pl.ds(SUM_BASE[p] // 8, SUM_ROWS[p] // 8), :]
            fin[t, SUM_BASE[p] // 8:(SUM_BASE[p] + SUM_ROWS[p]) // 8, :] = total
            place = out.at[out_slot(core, p, *bits(p), 1), :]
            keep = pltpu.make_async_copy(own, place, s_own.at[t])
            keep.start()
            for k in (2, 0, 1):
                send(own, place, s_g1.at[t], m_g1.at[t, k], plane_dev(p, k))
            send(own, place, s_g2.at[t], m_g2.at[t], dev(ORDERS[p][0]))

    def ag_plane(t, out):
        for k in range(3):
            arrived(out.at[0:HALF // 8, :], m_g1.at[t, k])
            for p in range(3):
                ref = plane_shard(out, p, k)
                send(ref, ref, s_g2.at[t], m_g2.at[t], dev(ORDERS[p][0]))
        pltpu.make_async_copy(fin.at[t], out.at[0:HALF // 8, :], s_own.at[t]).wait()
        for p in range(3):
            ref = axis_half(out, p, 0)
            send(ref, ref, s_fw.at[t], m_fw.at[t], partner)

    def ag_axis(t, out):
        arrived(out.at[0:HALF // 2, :], m_g2.at[t])
        for p in range(3):
            ref = axis_half(out, p, 1)
            send(ref, ref, s_fw.at[t], m_fw.at[t], partner)

    def ag_finish(t, out):
        arrived(out.at[0:HALF, :], m_fw.at[t])

    def sums_sent(t, out, pp, ra, rb):
        sent(pp, s_pair.at[t])
        sent(ra, s_r1.at[t])
        sent(rb, s_r2.at[t])
        sent(rb, s_g1.at[t])
        sent(ra, s_g2.at[t])
        sent(pp, s_fw.at[t])

    def dv_block(b, own=False):
        s = dot_nt(vall[me], uall[b])
        p = jnp.exp2(s * LOGIT_SCALE - wide(bcol[...])) * msgs[b, :, 0:ROWS]
        if own:
            p = jnp.where(eye, p - 1.0, p)
        return dot_nn(p.astype(BF16), uall[b])

    tower_backward(qx, wqo, a_q, h_q, u_q, r_q, gp_q)
    pair_start(0, gp_q, pp_q)
    gather_jobs(uall, 0, 2, s_u, m_u)
    pair_send(uall, 1, s_u.at[1], m_ud)
    dacc[...] = dv_block(me, True)
    gather_jobs(uall, 1, 1, s_u, m_u)
    pair_finish(0, gp_q, pp_q, ra_q)

    arrived(msgs.at[0:NDEV - 1], m_msg.at[0])
    total = msgs[0, :, ROWS:MSG]
    for b in range(1, NDEV):
        total = total + msgs[b, :, ROWS:MSG]
    loss_out[...] = jnp.broadcast_to(jnp.sum(total, axis=1, keepdims=True) * (1.0 / TOTAL), (1, 128))

    def dv_group(blocks):
        total = dacc[...]
        for b in blocks:
            total = total + dv_block(b)
        dacc[...] = total

    def dv_step(g, _):
        @pl.when(g == 1)
        def _():
            gather_jobs(uall, 1, 2, s_u, m_u)
            pair_send(uall, 2, s_u.at[1], m_ud)
            pair_wait(uall, 1, m_ud)

        @pl.when(g == 2)
        def _():
            r1_finish(0, pp_q, ra_q, rb_q)

        @pl.when(g == 3)
        def _():
            gather_jobs(uall, 2, 2, s_u, m_u)
            pair_send(uall, 3, s_u.at[1], m_ud)
            pair_wait(uall, 2, m_ud)

        @pl.when(g == 4)
        def _():
            pair_wait(uall, 3, m_ud)

        dv_group([nth_dev(3 * g + j) for j in range(3)])
        return 0

    pair_wait(uall, 0, m_ud)
    lax.fori_loop(0, 5, dv_step, 0)
    tower_backward(vx, wvo, a_v, h_v, u_v, r_v, gp_v)
    pair_start(1, gp_v, pp_v)
    r2_finish(0, gq_out, pp_q, rb_q)
    sent(vall.at[0:7], s_v.at[0])
    sent(lqall.at[0:7], s_v.at[1])
    sent(vall.at[0:8], s_v.at[2])
    sent(lqall.at[0:8], s_v.at[3])
    sent(uall.at[0:7], s_u.at[0])
    sent(uall.at[0:8], s_u.at[1])
    sent(msgs.at[0:NDEV - 1], s_msg.at[0])
    pair_finish(1, gp_v, pp_v, ra_v)
    ag_plane(0, gq_out)
    r1_finish(1, pp_v, ra_v, rb_v)
    ag_axis(0, gq_out)
    r2_finish(1, gv_out, pp_v, rb_v)
    ag_finish(0, gq_out)
    sums_sent(0, gq_out, pp_q, ra_q, rb_q)
    ag_plane(1, gv_out)
    ag_axis(1, gv_out)
    ag_finish(1, gv_out)
    sums_sent(1, gv_out, pp_v, ra_v, rb_v)


def finish(loss, gq, gv, loss_out, gqi, gqo, gvi, gvo, sem):
    copies = []
    for i, (g, gi, go) in enumerate(((gq, gqi, gqo), (gv, gvi, gvo))):
        copies.append(pltpu.make_async_copy(g.at[0:FEAT, :], gi.at[:, 0:EMB], sem.at[i, 0]))
        copies.append(pltpu.make_async_copy(g.at[FEAT:2 * FEAT, :], gi.at[:, EMB:HID], sem.at[i, 1]))
        copies.append(pltpu.make_async_copy(g.at[2 * FEAT:PACK, :], go, sem.at[i, 2]))
    for copy in copies:
        copy.start()
    loss_out[0] = loss[0, 0]
    for copy in copies:
        copy.wait()


def solution(mesh):
    vmem = pl.BlockSpec(memory_space=pltpu.VMEM)
    smem = pl.BlockSpec(memory_space=pltpu.SMEM)
    hbm = pl.BlockSpec(memory_space=pltpu.HBM)
    anym = pl.BlockSpec(memory_space=pl.ANY)
    dma = pltpu.SemaphoreType.DMA
    V = pltpu.VMEM

    def local_step(query_feat, item_feat, log_q, w_query_in, w_query_out, w_item_in, w_item_out):
        shape = jax.ShapeDtypeStruct
        loss, gq, gv = pl.pallas_call(
            kernel,
            out_shape=(shape((1, 128), F32), shape((PACK, EMB), F32), shape((PACK, EMB), F32)),
            in_specs=[hbm] * 7,
            out_specs=(vmem, anym, anym),
            scratch_shapes=[
                V((ROWS, FEAT), BF16), V((ROWS, FEAT), BF16),
                V((FEAT, HID), BF16), V((HID, EMB), BF16), V((FEAT, HID), BF16), V((HID, EMB), BF16), dma((7,)),
                V((NDEV, ROWS, EMB), BF16), V((NDEV, ROWS, EMB), BF16),
                V((NDEV, 1, ROWS), F32), V((1, 128), F32), V((1, ROWS), F32),
                V((NDEV, 1, MSG), F32),
                V((ROWS, EMB), F32), V((ROWS, EMB), F32),
                V((ROWS, HID), F32), V((ROWS, HID), F32),
                V((ROWS, HID), BF16), V((ROWS, HID), BF16),
                V((ROWS, EMB), F32), V((ROWS, EMB), F32),
                V((ROWS, EMB), F32), V((ROWS, EMB), F32),
                V((ROWS, EMB), F32), V((ROWS, EMB), F32), V((ROWS, EMB), F32),
                V((PACK, EMB), F32), V((PACK, EMB), F32),
                V((HALF, EMB), F32), V((HALF, EMB), F32),
                V((HALF // 2, EMB), F32), V((HALF // 2, EMB), F32),
                V((3, HALF // 8, EMB), F32), V((3, HALF // 8, EMB), F32), V((2, HALF // 8, EMB), F32), dma((2,)),
                dma((1,)), dma((1,)),
                dma((4,)), dma((6,)), dma((8,)), dma((4,)), dma((4,)), dma((2,)), dma((6,)), dma((4,)),
                dma((2,)), dma((2,)), dma((2,)), dma((2,)), dma((2,)), dma((2,)),
                dma((2,)), dma((2, 3)), dma((2,)), dma((2,)), dma((2,)), dma((2,)),
            ],
            compiler_params=pltpu.CompilerParams(collective_id=0, has_side_effects=True,
                                                 vmem_limit_bytes=48 * 1024 * 1024),
            name="step",
        )(*(pltpu.with_memory_space_constraint(x, pltpu.HBM) for x in (
            query_feat, item_feat, log_q.reshape(1, ROWS), w_query_in, w_query_out, w_item_in, w_item_out)))
        return pl.pallas_call(
            finish,
            out_shape=(shape((1,), F32), shape((FEAT, HID), F32), shape((HID, EMB), F32),
                       shape((FEAT, HID), F32), shape((HID, EMB), F32)),
            in_specs=[vmem, anym, anym],
            out_specs=(smem, hbm, hbm, hbm, hbm),
            scratch_shapes=[dma((2, 3))],
            compiler_params=pltpu.CompilerParams(vmem_limit_bytes=8 * 1024 * 1024),
            name="finish",
        )(loss, gq, gv)

    return jax.shard_map(local_step, mesh=mesh, in_specs=(P('dp', None), P('dp', None), P('dp'), P(), P(), P(), P()), out_specs=(P(), P(), P(), P(), P()), check_vma=False)
```

```python
import jax
import jax.numpy as jnp
from jax import lax
from jax.experimental import pallas as pl
from jax.experimental.pallas import tpu as pltpu
from jax.sharding import PartitionSpec as P

MESH = pl.DeviceIdType.MESH
TEMPERATURE = 0.05
NORM_EPS = 1e-6
LOG2E = 1.4426950408889634
NDEV = 16
ROWS = 512
FEAT = 512
HID = 256
EMB = 128
PACK = 2 * FEAT + HID
HALF = PACK // 2
SUM_BASE = (0, 448, 896)
SUM_ROWS = (448, 448, 384)
TOTAL = NDEV * ROWS
GRAD_SCALE = 1.0 / (TEMPERATURE * TOTAL)
LOGIT_SCALE = LOG2E / TEMPERATURE
PARTS = ((0, 176), (176, 176), (352, 160))
ORDERS = ((1, 2, 4), (2, 4, 1), (4, 1, 2), (1, 2, 4))
LEVELS = ((1, 2, 4), (6, 5, 3), (7,))
PAIR = ((0,),) + LEVELS
SLOT = {(0, 0): 0, (0, 1): 1, (0, 2): 2, (1, 1): 3, (1, 2): 4, (2, 2): 5}
MSG = ROWS + 128
F32 = jnp.float32
BF16 = jnp.bfloat16


def dot_nn(a, b):
    return lax.dot_general(a, b, (((1,), (0,)), ((), ())), preferred_element_type=F32)


def dot_nt(a, b):
    return lax.dot_general(a, b, (((1,), (1,)), ((), ())), preferred_element_type=F32)


def dot_tn(a, b):
    return lax.dot_general(a, b, (((0,), (0,)), ((), ())), preferred_element_type=F32)


def wide(col):
    return jnp.concatenate([col] * (ROWS // EMB), axis=1)


def kernel(qx_h, vx_h, lq_h, wqi_h, wqo_h, wvi_h, wvo_h,
           loss_out, gq_out, gv_out,
           qx, vx, wqi, wqo, wvi, wvo, s_in,
           uall, vall, lqall, crun, pos_row, msgs, lacc, diag, invl, bcol, dacc,
           a_q, a_v, h_q, h_v, u_q, u_v, r_q, r_v,
           gp_q, gp_v, pp, ra, rb, fin, s_own,
           s_msg, m_msg,
           s_v, m_v, m_l, m_vd, m_ld, s_u, m_u, m_ud,
           s_pair, m_pair, s_r1, m_r1, s_r2, m_r2, s_g1, m_g1, s_g2, m_g2, s_fw, m_fw):
    me = lax.axis_index("dp")
    core = me % 2
    bit_x, bit_y, bit_z = (me // 2) % 2, (me // 4) % 2, (me // 8) % 2
    step_x, step_y, step_z = 2 - 4 * bit_x, 4 - 8 * bit_y, 8 - 16 * bit_z
    partner = me + 1 - 2 * core
    chip = me // 2

    def flipped(mask):
        return me + (mask % 2) * step_x + ((mask // 2) % 2) * step_y + (mask // 4) * step_z

    same_core = [flipped(mask) for mask in range(8)]

    def dev(mask):
        return same_core[mask]

    def dev_other(mask):
        return same_core[mask] + partner - me

    def nth_dev(n):
        q, r = (n + 2) // 3, (n + 2) % 3
        base = r * (r + 1) // 2 + 1
        last = q // 5
        mask = (base + q // 3 * (7 - 2 * base)) * ((q + 4) // 5) * (1 - last) + 7 * last
        return flipped(mask) + ((q + 1) % 2 + last * (n - 13)) * (partner - me)

    def rcopy(src, dst, ssem, rsem, to):
        return pltpu.make_async_remote_copy(src_ref=src, dst_ref=dst, send_sem=ssem, recv_sem=rsem,
                                            device_id=(to,), device_id_type=MESH)

    def send(src, dst, ssem, rsem, to):
        rcopy(src, dst, ssem, rsem, to).start()

    def sent(like, ssem):
        rcopy(like, like, ssem, ssem, partner).wait_send()

    def arrived(ref, rsem):
        rcopy(ref, ref, rsem, rsem, partner).wait_recv()

    others = [(me + k) % NDEV for k in range(1, NDEV)]

    loads = [pltpu.make_async_copy(src, dst, s_in.at[i]) for i, (src, dst) in enumerate((
        (vx_h, vx), (wvi_h, wvi), (wvo_h, wvo), (lq_h, lqall.at[me]), (qx_h, qx), (wqi_h, wqi), (wqo_h, wqo)))]
    for load in loads:
        load.start()
    barrier = pltpu.get_barrier_semaphore()
    for to in (partner, dev(1), dev(2), dev(4)):
        pl.semaphore_signal(barrier, inc=1, device_id=(to,), device_id_type=MESH)

    def tower_forward(x, w_in, w_out, a_ref, h_ref, u_ref, r_ref, all_ref):
        a = dot_nn(x[...], w_in[...])
        a_ref[...] = a
        h = jnp.maximum(a, 0.0).astype(BF16)
        h_ref[...] = h
        e = dot_nn(h, w_out[...])
        r = lax.rsqrt(jnp.sum(e * e, axis=-1, keepdims=True) + NORM_EPS)
        u = e * r
        u_ref[...] = u
        r_ref[...] = jnp.broadcast_to(r, (ROWS, EMB))
        all_ref[me] = u.astype(BF16)

    for load in loads[:4]:
        load.wait()
    tower_forward(vx, wvi, wvo, a_v, h_v, u_v, r_v, vall)
    pl.semaphore_wait(barrier, 4)

    def part_ref(ref, src, p):
        if p == 3:
            return lqall.at[src]
        return ref.at[src, pl.ds(PARTS[p][0], PARTS[p][1]), :]

    def send_part(ref, p, m, t, ss, ms):
        d = ORDERS[p][t]
        src = part_ref(ref, dev(m), p)
        to = m + d
        rsem = ms.at[to] if p == 3 else ms.at[SLOT[bin(to).count("1") - 1, top_turn(p, to)]]
        send(src, src, ss.at[p // 3], rsem, dev(d))

    def gather_own(ref, ts, ss, ms):
        for t in ts:
            for p in range(3):
                send_part(ref, p, 0, t, ss, ms)

    def top_turn(p, m):
        return max(t for t in range(3) if ORDERS[p][t] & m)

    def gather_jobs(ref, level, t, ss, ms, ml=None):
        jobs = [(p, m) for p in range(3) for m in LEVELS[level] if top_turn(p, m) == t]
        arrived(ref.at[0:len(jobs) // 3] if len(jobs) > 3 else ref.at[0], ms.at[SLOT[level, t]])
        if ml is not None:
            for m in sorted({m for m in LEVELS[level] if top_turn(3, m) == t}):
                arrived(lqall.at[dev(m)], ml.at[m])
                for tt in range(t + 1, 3):
                    send_part(lqall, 3, m, tt, ss, ml)
        for tt in range(t + 1, 3):
            for p, m in jobs:
                send_part(ref, p, m, tt, ss, ms)

    def pair_send(ref, level, sd, md):
        for m in PAIR[level]:
            send(ref.at[dev(m)], ref.at[dev(m)], sd, md.at[level], partner)

    def pair_wait(ref, level, md):
        arrived(ref.at[0:len(PAIR[level])], md.at[level])

    pair_send(lqall, 0, s_v.at[3], m_ld)
    pair_send(vall, 0, s_v.at[2], m_vd)
    for t in range(3):
        send_part(lqall, 3, 0, t, s_v, m_l)
    gather_own(vall, (0, 1, 2), s_v, m_v)

    for load in loads[4:]:
        load.wait()
    tower_forward(qx, wqi, wqo, a_q, h_q, u_q, r_q, uall)
    pair_send(uall, 0, s_u.at[1], m_ud)

    eye = (lax.broadcasted_iota(jnp.int32, (ROWS, ROWS), 0)
           == lax.broadcasted_iota(jnp.int32, (ROWS, ROWS), 1))

    def block_shift(b):
        return jnp.max(-lqall[b], axis=1, keepdims=True)

    def exp_block(b, c):
        s = dot_nt(uall[me], vall[b])
        return jnp.exp2(s * LOGIT_SCALE - (lqall[b] + c) * LOG2E)

    def lane_sum(e):
        return e[:, 0:128] + e[:, 128:256] + (e[:, 256:384] + e[:, 384:512])

    def exp_group(blocks):
        c_old = crun[...]
        c = c_old
        for b in blocks:
            c = jnp.maximum(c, block_shift(b))
        crun[...] = c
        scale = jnp.exp2((c_old - c) * LOG2E)
        l_new, d_new = lacc[...] * scale, dacc[...] * scale
        for b in blocks:
            e = exp_block(b, c[:, 0:1])
            l_new = l_new + lane_sum(e)
            d_new = d_new + dot_nn(e.astype(BF16), vall[b])
        lacc[...], dacc[...] = l_new, d_new

    c_own = block_shift(me)
    crun[...] = jnp.broadcast_to(c_own, (1, 128))
    e_own = exp_block(me, c_own)
    lacc[...] = lane_sum(e_own)
    diag[...] = jnp.broadcast_to(jnp.sum(jnp.where(eye, e_own, 0.0), axis=1, keepdims=True), (ROWS, EMB))
    dacc[...] = dot_nn(jnp.where(eye, 0.0, e_own).astype(BF16), vall[me])
    pos_row[...] = jnp.sum((uall[me].astype(F32) * vall[me].astype(F32)).T, axis=0, keepdims=True) * (1.0 / TEMPERATURE)

    def exp_step(g, _):
        @pl.when(g == 0)
        def _():
            for t in range(3):
                gather_jobs(vall, 0, t, s_v, m_v, m_l)
            pair_send(lqall, 1, s_v.at[3], m_ld)
            pair_send(vall, 1, s_v.at[2], m_vd)
            pair_wait(lqall, 0, m_ld)
            pair_wait(vall, 0, m_vd)
            gather_own(uall, (0,), s_u, m_u)

        @pl.when(g == 1)
        def _():
            gather_jobs(vall, 1, 1, s_v, m_v, m_l)
            gather_own(uall, (1, 2), s_u, m_u)
            pair_wait(lqall, 1, m_ld)
            pair_wait(vall, 1, m_vd)

        @pl.when(g == 2)
        def _():
            gather_jobs(vall, 1, 2, s_v, m_v, m_l)
            pair_send(lqall, 2, s_v.at[3], m_ld)
            pair_send(vall, 2, s_v.at[2], m_vd)

        @pl.when(g == 3)
        def _():
            gather_jobs(vall, 2, 2, s_v, m_v, m_l)
            pair_send(lqall, 3, s_v.at[3], m_ld)
            pair_send(vall, 3, s_v.at[2], m_vd)
            pair_wait(lqall, 2, m_ld)
            pair_wait(vall, 2, m_vd)

        @pl.when(g == 4)
        def _():
            gather_jobs(uall, 0, 0, s_u, m_u)
            pair_wait(lqall, 3, m_ld)
            pair_wait(vall, 3, m_vd)

        exp_group([nth_dev(3 * g + j) for j in range(3)])
        return 0

    lax.fori_loop(0, 5, exp_step, 0)

    acc = lacc[...]
    shift = crun[0:1, 0:1]
    lq_own = lqall[me]
    l_row = jnp.sum(acc.T, axis=0, keepdims=True)
    loss_row = jnp.log(l_row) + ((shift + lq_own) - pos_row[...])
    loss_part = loss_row[:, 0:128] + loss_row[:, 128:256] + (loss_row[:, 256:384] + loss_row[:, 384:512])
    msgs[me, :, 0:ROWS] = 1.0 / l_row
    msgs[me, :, ROWS:MSG] = loss_part
    for k in range(NDEV - 1):
        send(msgs.at[me], msgs.at[me], s_msg.at[0], m_msg.at[0], others[k])
    invl[...] = jnp.broadcast_to(1.0 / jnp.sum(acc, axis=1, keepdims=True), (ROWS, EMB))
    bcol[...] = jnp.broadcast_to((lq_own + shift) * LOG2E, (EMB, ROWS)).T

    p_own = diag[...] * jnp.exp2((c_own - crun[...]) * LOG2E) * invl[...]
    dacc[...] = dacc[...] * invl[...] + (p_own - 1.0).astype(BF16).astype(F32) * vall[me].astype(F32)
    gather_jobs(uall, 0, 1, s_u, m_u)

    def tower_backward(owner, x, w_out, a_ref, h_ref, u_ref, r_ref, g):
        d_unit = dacc[...] * GRAD_SCALE
        u = u_ref[...]
        de = (r_ref[...] * (d_unit - u * jnp.sum(u * d_unit, axis=-1, keepdims=True))).astype(BF16)
        g[2 * FEAT:PACK, :] = dot_tn(h_ref[...], de)
        hand_over(owner, g, GO)
        dh = dot_nt(de, w_out[...])
        da = jnp.where(a_ref[...] > 0, dh, 0.0).astype(BF16)
        gi = dot_tn(x[...], da)
        g[0:FEAT, :] = gi[:, 0:EMB]
        g[FEAT:2 * FEAT, :] = gi[:, EMB:HID]
        hand_over(owner, g, GI)

    bit = {1: bit_x, 2: bit_y, 4: bit_z}
    PLANE = ((0, 1), (1, 0), (1, 1))

    def slot(p, b0, b1, b2, count):
        eighth = SUM_ROWS[p] // 8
        return pl.ds(pl.multiple_of(SUM_BASE[p] + (b0 * 4 + b1 * 2 + b2) * eighth, 8), count * eighth)

    def part(p, share):
        return pl.ds(SUM_BASE[p] // share, SUM_ROWS[p] // share)

    def bits(p, flip=(0, 0)):
        b = [bit[d] for d in ORDERS[p]]
        return (b[0],) + tuple(1 - v if f else v for v, f in zip(b[1:], flip))

    def plane_dev(p, k):
        return dev(PLANE[k][0] * ORDERS[p][1] + PLANE[k][1] * ORDERS[p][2])

    def plane_shard(out, p, k):
        return out.at[slot(p, *bits(p, PLANE[k]), 1), :]

    def axis_half(out, p, far):
        b0 = bits(p)[0]
        return out.at[slot(p, 1 - b0 if far else b0, 0, 0, 4), :]

    GO, GI = pl.ds(2 * FEAT, HID), pl.ds(0, 2 * FEAT)

    def hand_over(owner, g, rows):
        @pl.when(core != owner)
        def _():
            send(g.at[rows, :], pp.at[rows, :], s_pair, m_pair, partner)

    def sum_pair(g):
        arrived(pp, m_pair)
        pp[...] = pp[...] + g[...]
        for p in range(3):
            send(pp.at[slot(p, 1 - bits(p)[0], 0, 0, 4), :], ra.at[part(p, 2), :], s_r1, m_r1, dev(ORDERS[p][0]))

    def sum_axis():
        arrived(ra, m_r1)
        for p in range(3):
            mine = slot(p, bits(p)[0], 0, 0, 4)
            pp[mine, :] = pp[mine, :] + ra[part(p, 2), :]
        for k in (2, 0, 1):
            for p in range(3):
                send(pp.at[slot(p, *bits(p, PLANE[k]), 1), :], rb.at[k, part(p, 8), :], s_r2, m_r2, plane_dev(p, k))

    def sum_plane(out):
        arrived(rb, m_r2)
        for p in range(3):
            total = pp[slot(p, *bits(p), 1), :]
            for k in range(3):
                total = total + rb[k, part(p, 8), :]
            fin[part(p, 8), :] = total
        for k in (2, 0, 1):
            for p in range(3):
                send(fin.at[part(p, 8), :], out.at[slot(p, *bits(p), 1), :], s_g1, m_g1.at[k], plane_dev(p, k))
        for p in range(3):
            place = out.at[slot(p, *bits(p), 1), :]
            send(fin.at[part(p, 8), :], place, s_g2, m_g2, dev(ORDERS[p][0]))
            pltpu.make_async_copy(fin.at[part(p, 8), :], place, s_own).start()

    def spread_plane(out):
        for k in range(3):
            arrived(fin, m_g1.at[k])
            for p in range(3):
                ref = plane_shard(out, p, k)
                send(ref, ref, s_g2, m_g2, dev(ORDERS[p][0]))
        pltpu.make_async_copy(fin, out.at[part(0, 1), :].at[0:HALF // 4, :], s_own).wait()
        for p in range(3):
            ref = axis_half(out, p, 0)
            send(ref, ref, s_fw, m_fw, partner)

    def spread_axis(out):
        arrived(ra, m_g2)
        for p in range(3):
            ref = axis_half(out, p, 1)
            send(ref, ref, s_fw, m_fw, partner)

    def on_core(owner, stage, *args):
        @pl.when(core == owner)
        def _():
            stage(*args)

    def dv_block(b, own=False):
        s = dot_nt(vall[me], uall[b])
        p = jnp.exp2(s * LOGIT_SCALE - wide(bcol[...])) * msgs[b, :, 0:ROWS]
        if own:
            p = jnp.where(eye, p - 1.0, p)
        return dot_nn(p.astype(BF16), uall[b])

    tower_backward(0, qx, wqo, a_q, h_q, u_q, r_q, gp_q)
    gather_jobs(uall, 0, 2, s_u, m_u)
    pair_send(uall, 1, s_u.at[1], m_ud)
    dacc[...] = dv_block(me, True)
    gather_jobs(uall, 1, 1, s_u, m_u)
    on_core(0, sum_pair, gp_q)

    arrived(msgs.at[0:NDEV - 1], m_msg.at[0])
    total = msgs[0, :, ROWS:MSG]
    for b in range(1, NDEV):
        total = total + msgs[b, :, ROWS:MSG]
    loss_out[...] = jnp.broadcast_to(jnp.sum(total, axis=1, keepdims=True) * (1.0 / TOTAL), (1, 128))

    def dv_group(blocks):
        total = dacc[...]
        for b in blocks:
            total = total + dv_block(b)
        dacc[...] = total

    def dv_step(g, _):
        @pl.when(g == 1)
        def _():
            gather_jobs(uall, 1, 2, s_u, m_u)
            pair_send(uall, 2, s_u.at[1], m_ud)
            pair_wait(uall, 1, m_ud)

        @pl.when(g == 2)
        def _():
            on_core(0, sum_axis)

        @pl.when(g == 3)
        def _():
            gather_jobs(uall, 2, 2, s_u, m_u)
            pair_send(uall, 3, s_u.at[1], m_ud)
            pair_wait(uall, 2, m_ud)

        @pl.when(g == 4)
        def _():
            pair_wait(uall, 3, m_ud)

        dv_group([nth_dev(3 * g + j) for j in range(3)])
        return 0

    pair_wait(uall, 0, m_ud)
    lax.fori_loop(0, 5, dv_step, 0)
    tower_backward(1, vx, wvo, a_v, h_v, u_v, r_v, gp_v)
    on_core(0, sum_plane, gq_out)
    sent(vall.at[0:7], s_v.at[0])
    sent(lqall.at[0:7], s_v.at[1])
    sent(vall.at[0:8], s_v.at[2])
    sent(lqall.at[0:8], s_v.at[3])
    sent(uall.at[0:7], s_u.at[0])
    sent(uall.at[0:8], s_u.at[1])
    sent(msgs.at[0:NDEV - 1], s_msg.at[0])
    on_core(1, sum_pair, gp_v)
    on_core(0, spread_plane, gq_out)
    on_core(1, sum_axis)
    on_core(0, spread_axis, gq_out)
    on_core(1, sum_plane, gv_out)
    on_core(1, spread_plane, gv_out)
    on_core(1, spread_axis, gv_out)
    sent(pp, s_pair)
    for like, ssem in ((ra, s_r1), (rb, s_r2), (rb, s_g1), (ra, s_g2), (pp, s_fw)):
        sent(like, ssem)
    arrived(pp, m_fw)


def finish(loss, gq, gv, loss_out, gqi, gqo, gvi, gvo, sem):
    copies = []
    for i, (g, gi, go) in enumerate(((gq, gqi, gqo), (gv, gvi, gvo))):
        copies.append(pltpu.make_async_copy(g.at[0:FEAT, :], gi.at[:, 0:EMB], sem.at[i, 0]))
        copies.append(pltpu.make_async_copy(g.at[FEAT:2 * FEAT, :], gi.at[:, EMB:HID], sem.at[i, 1]))
        copies.append(pltpu.make_async_copy(g.at[2 * FEAT:PACK, :], go, sem.at[i, 2]))
    for copy in copies:
        copy.start()
    loss_out[0] = loss[0, 0]
    for copy in copies:
        copy.wait()


def solution(mesh):
    vmem = pl.BlockSpec(memory_space=pltpu.VMEM)
    smem = pl.BlockSpec(memory_space=pltpu.SMEM)
    hbm = pl.BlockSpec(memory_space=pltpu.HBM)
    anym = pl.BlockSpec(memory_space=pl.ANY)
    dma = pltpu.SemaphoreType.DMA
    V = pltpu.VMEM

    def local_step(query_feat, item_feat, log_q, w_query_in, w_query_out, w_item_in, w_item_out):
        shape = jax.ShapeDtypeStruct
        loss, gq, gv = pl.pallas_call(
            kernel,
            out_shape=(shape((1, 128), F32), shape((PACK, EMB), F32), shape((PACK, EMB), F32)),
            in_specs=[hbm] * 7,
            out_specs=(vmem, anym, anym),
            scratch_shapes=(
                [V((ROWS, FEAT), BF16)] * 2 + [V((FEAT, HID), BF16), V((HID, EMB), BF16)] * 2 + [dma((7,))]
                + [V((NDEV, ROWS, EMB), BF16)] * 2
                + [V((NDEV, 1, ROWS), F32), V((1, EMB), F32), V((1, ROWS), F32), V((NDEV, 1, MSG), F32)]
                + [V((ROWS, EMB), F32)] * 5
                + [V((ROWS, HID), F32)] * 2 + [V((ROWS, HID), BF16)] * 2 + [V((ROWS, EMB), F32)] * 4
                + [V((PACK, EMB), F32)] * 3 + [V((HALF, EMB), F32), V((3, HALF // 4, EMB), F32), V((HALF // 4, EMB), F32)]
                + [dma]
                + [dma((1,))] * 2 + [dma((n,)) for n in (4, 6, 8, 4, 4, 2, 6, 4)]
                + [dma] * 7 + [dma((3,))] + [dma] * 4),
            compiler_params=pltpu.CompilerParams(collective_id=0, has_side_effects=True,
                                                 vmem_limit_bytes=48 * 1024 * 1024),
            name="step",
        )(*(pltpu.with_memory_space_constraint(x, pltpu.HBM) for x in (
            query_feat, item_feat, log_q.reshape(1, ROWS), w_query_in, w_query_out, w_item_in, w_item_out)))
        return pl.pallas_call(
            finish,
            out_shape=(shape((1,), F32), shape((FEAT, HID), F32), shape((HID, EMB), F32),
                       shape((FEAT, HID), F32), shape((HID, EMB), F32)),
            in_specs=[vmem, anym, anym],
            out_specs=(smem, hbm, hbm, hbm, hbm),
            scratch_shapes=[dma((2, 3))],
            compiler_params=pltpu.CompilerParams(vmem_limit_bytes=8 * 1024 * 1024),
            name="finish",
        )(loss, gq, gv)

    return jax.shard_map(local_step, mesh=mesh, in_specs=(P('dp', None), P('dp', None), P('dp'), P(), P(), P(), P()), out_specs=(P(), P(), P(), P(), P()), check_vma=False)
```

```python
import jax
import jax.numpy as jnp
from jax import lax
from jax.experimental import pallas as pl
from jax.experimental.pallas import tpu as pltpu
from jax.sharding import PartitionSpec as P

MESH = pl.DeviceIdType.MESH
TEMPERATURE = 0.05
NORM_EPS = 1e-6
LOG2E = 1.4426950408889634
NDEV = 16
ROWS = 512
FEAT = 512
HID = 256
EMB = 128
PACK = 2 * FEAT + HID
HALF = PACK // 2
SUM_BASE = (0, 448, 896)
SUM_ROWS = (448, 448, 384)
TOTAL = NDEV * ROWS
GRAD_SCALE = 1.0 / (TEMPERATURE * TOTAL)
LOGIT_SCALE = LOG2E / TEMPERATURE
PARTS = ((0, 176), (176, 176), (352, 160))
ORDERS = ((1, 2, 4), (2, 4, 1), (4, 1, 2), (1, 2, 4))
LEVELS = ((1, 2, 4), (6, 5, 3), (7,))
PAIR = ((0,),) + LEVELS
SLOT = {(0, 0): 0, (0, 1): 1, (0, 2): 2, (1, 1): 3, (1, 2): 4, (2, 2): 5}
MSG = ROWS + 128
F32 = jnp.float32
BF16 = jnp.bfloat16


def dot_nn(a, b):
    return lax.dot_general(a, b, (((1,), (0,)), ((), ())), preferred_element_type=F32)


def dot_nt(a, b):
    return lax.dot_general(a, b, (((1,), (1,)), ((), ())), preferred_element_type=F32)


def dot_tn(a, b):
    return lax.dot_general(a, b, (((0,), (0,)), ((), ())), preferred_element_type=F32)


def wide(col):
    return jnp.concatenate([col] * (ROWS // EMB), axis=1)


def kernel(qx_h, vx_h, lq_h, wqi_h, wqo_h, wvi_h, wvo_h,
           loss_out, gq_out, gv_out,
           qx, vx, wqi, wqo, wvi, wvo, s_in,
           uall, vall, lqall, crun, pos_row, msgs, lacc, diag, invl, bcol, dacc,
           a_q, a_v, h_q, h_v, u_q, u_v, r_q, r_v,
           gp_q, gp_v, pp, ra, rb, fin, s_own,
           s_msg, m_msg,
           s_v, m_v, m_l, m_vd, m_ld, s_u, m_u, m_ud,
           s_pair, m_pair, s_r1, m_r1, s_r2, m_r2, s_g1, m_g1, s_g2, m_g2, s_fw, m_fw):
    me = lax.axis_index("dp")
    core = me % 2
    bit_x, bit_y, bit_z = (me // 2) % 2, (me // 4) % 2, (me // 8) % 2
    step_x, step_y, step_z = 2 - 4 * bit_x, 4 - 8 * bit_y, 8 - 16 * bit_z
    partner = me + 1 - 2 * core
    chip = me // 2

    def flipped(mask):
        return me + (mask % 2) * step_x + ((mask // 2) % 2) * step_y + (mask // 4) * step_z

    same_core = [flipped(mask) for mask in range(8)]

    def dev(mask):
        return same_core[mask]

    def dev_other(mask):
        return same_core[mask] + partner - me

    def nth_dev(n):
        q, r = (n + 2) // 3, (n + 2) % 3
        base = r * (r + 1) // 2 + 1
        last = q // 5
        mask = (base + q // 3 * (7 - 2 * base)) * ((q + 4) // 5) * (1 - last) + 7 * last
        return flipped(mask) + ((q + 1) % 2 + last * (n - 13)) * (partner - me)

    def rcopy(src, dst, ssem, rsem, to):
        return pltpu.make_async_remote_copy(src_ref=src, dst_ref=dst, send_sem=ssem, recv_sem=rsem,
                                            device_id=(to,), device_id_type=MESH)

    def send(src, dst, ssem, rsem, to):
        rcopy(src, dst, ssem, rsem, to).start()

    def sent(like, ssem):
        rcopy(like, like, ssem, ssem, partner).wait_send()

    def arrived(ref, rsem):
        rcopy(ref, ref, rsem, rsem, partner).wait_recv()

    others = [(me + k) % NDEV for k in range(1, NDEV)]

    loads = [pltpu.make_async_copy(src, dst, s_in.at[i]) for i, (src, dst) in enumerate((
        (vx_h, vx), (wvi_h, wvi), (wvo_h, wvo), (lq_h, lqall.at[me]), (qx_h, qx), (wqi_h, wqi), (wqo_h, wqo)))]
    for load in loads:
        load.start()
    barrier = pltpu.get_barrier_semaphore()
    for to in (partner, dev(1), dev(2), dev(4)):
        pl.semaphore_signal(barrier, inc=1, device_id=(to,), device_id_type=MESH)

    def tower_forward(x, w_in, w_out, a_ref, h_ref, u_ref, r_ref, all_ref):
        a = dot_nn(x[...], w_in[...])
        a_ref[...] = a
        h = jnp.maximum(a, 0.0).astype(BF16)
        h_ref[...] = h
        e = dot_nn(h, w_out[...])
        r = lax.rsqrt(jnp.sum(e * e, axis=-1, keepdims=True) + NORM_EPS)
        u = e * r
        u_ref[...] = u
        r_ref[...] = jnp.broadcast_to(r, (ROWS, EMB))
        all_ref[me] = u.astype(BF16)

    for load in loads[:4]:
        load.wait()
    tower_forward(vx, wvi, wvo, a_v, h_v, u_v, r_v, vall)
    pl.semaphore_wait(barrier, 4)

    def part_ref(ref, src, p):
        if p == 3:
            return lqall.at[src]
        return ref.at[src, pl.ds(PARTS[p][0], PARTS[p][1]), :]

    def send_part(ref, p, m, t, ss, ms):
        d = ORDERS[p][t]
        src = part_ref(ref, dev(m), p)
        to = m + d
        rsem = ms.at[to] if p == 3 else ms.at[SLOT[bin(to).count("1") - 1, top_turn(p, to)]]
        send(src, src, ss.at[p // 3], rsem, dev(d))

    def gather_own(ref, ts, ss, ms):
        for t in ts:
            for p in range(3):
                send_part(ref, p, 0, t, ss, ms)

    def top_turn(p, m):
        return max(t for t in range(3) if ORDERS[p][t] & m)

    def gather_jobs(ref, level, t, ss, ms, ml=None):
        jobs = [(p, m) for p in range(3) for m in LEVELS[level] if top_turn(p, m) == t]
        arrived(ref.at[0:len(jobs) // 3] if len(jobs) > 3 else ref.at[0], ms.at[SLOT[level, t]])
        if ml is not None:
            for m in sorted({m for m in LEVELS[level] if top_turn(3, m) == t}):
                arrived(lqall.at[dev(m)], ml.at[m])
                for tt in range(t + 1, 3):
                    send_part(lqall, 3, m, tt, ss, ml)
        for tt in range(t + 1, 3):
            for p, m in jobs:
                send_part(ref, p, m, tt, ss, ms)

    def pair_send(ref, level, sd, md):
        for m in PAIR[level]:
            send(ref.at[dev(m)], ref.at[dev(m)], sd, md.at[level], partner)

    def pair_wait(ref, level, md):
        arrived(ref.at[0:len(PAIR[level])], md.at[level])

    pair_send(lqall, 0, s_v.at[3], m_ld)
    pair_send(vall, 0, s_v.at[2], m_vd)
    for t in range(3):
        send_part(lqall, 3, 0, t, s_v, m_l)
    gather_own(vall, (0, 1, 2), s_v, m_v)

    for load in loads[4:]:
        load.wait()
    tower_forward(qx, wqi, wqo, a_q, h_q, u_q, r_q, uall)
    pair_send(uall, 0, s_u.at[1], m_ud)

    eye = (lax.broadcasted_iota(jnp.int32, (ROWS, ROWS), 0)
           == lax.broadcasted_iota(jnp.int32, (ROWS, ROWS), 1))

    def block_shift(b):
        return jnp.max(-lqall[b], axis=1, keepdims=True)

    def exp_block(b, c):
        s = dot_nt(uall[me], vall[b])
        return jnp.exp2(s * LOGIT_SCALE - (lqall[b] + c) * LOG2E)

    def lane_sum(e):
        return e[:, 0:128] + e[:, 128:256] + (e[:, 256:384] + e[:, 384:512])

    def exp_group(blocks):
        c_old = crun[...]
        c = c_old
        for b in blocks:
            c = jnp.maximum(c, block_shift(b))
        crun[...] = c
        scale = jnp.exp2((c_old - c) * LOG2E)
        l_new, d_new = lacc[...] * scale, dacc[...] * scale
        for b in blocks:
            e = exp_block(b, c[:, 0:1])
            l_new = l_new + lane_sum(e)
            d_new = d_new + dot_nn(e.astype(BF16), vall[b])
        lacc[...], dacc[...] = l_new, d_new

    c_own = block_shift(me)
    crun[...] = jnp.broadcast_to(c_own, (1, 128))
    e_own = exp_block(me, c_own)
    lacc[...] = lane_sum(e_own)
    diag[...] = jnp.broadcast_to(jnp.sum(jnp.where(eye, e_own, 0.0), axis=1, keepdims=True), (ROWS, EMB))
    dacc[...] = dot_nn(jnp.where(eye, 0.0, e_own).astype(BF16), vall[me])
    pos_row[...] = jnp.sum((uall[me].astype(F32) * vall[me].astype(F32)).T, axis=0, keepdims=True) * (1.0 / TEMPERATURE)

    def exp_step(g, _):
        @pl.when(g == 0)
        def _():
            for t in range(3):
                gather_jobs(vall, 0, t, s_v, m_v, m_l)
            pair_send(lqall, 1, s_v.at[3], m_ld)
            pair_send(vall, 1, s_v.at[2], m_vd)
            pair_wait(lqall, 0, m_ld)
            pair_wait(vall, 0, m_vd)
            gather_own(uall, (0,), s_u, m_u)

        @pl.when(g == 1)
        def _():
            gather_jobs(vall, 1, 1, s_v, m_v, m_l)
            gather_own(uall, (1, 2), s_u, m_u)
            pair_wait(lqall, 1, m_ld)
            pair_wait(vall, 1, m_vd)

        @pl.when(g == 2)
        def _():
            gather_jobs(vall, 1, 2, s_v, m_v, m_l)
            pair_send(lqall, 2, s_v.at[3], m_ld)
            pair_send(vall, 2, s_v.at[2], m_vd)

        @pl.when(g == 3)
        def _():
            gather_jobs(vall, 2, 2, s_v, m_v, m_l)
            pair_send(lqall, 3, s_v.at[3], m_ld)
            pair_send(vall, 3, s_v.at[2], m_vd)
            pair_wait(lqall, 2, m_ld)
            pair_wait(vall, 2, m_vd)

        @pl.when(g == 4)
        def _():
            gather_jobs(uall, 0, 0, s_u, m_u)
            pair_wait(lqall, 3, m_ld)
            pair_wait(vall, 3, m_vd)

        exp_group([nth_dev(3 * g + j) for j in range(3)])
        return 0

    lax.fori_loop(0, 5, exp_step, 0)

    acc = lacc[...]
    shift = crun[0:1, 0:1]
    lq_own = lqall[me]
    l_row = jnp.sum(acc.T, axis=0, keepdims=True)
    loss_row = jnp.log(l_row) + ((shift + lq_own) - pos_row[...])
    loss_part = loss_row[:, 0:128] + loss_row[:, 128:256] + (loss_row[:, 256:384] + loss_row[:, 384:512])
    msgs[me, :, 0:ROWS] = 1.0 / l_row
    msgs[me, :, ROWS:MSG] = loss_part
    for k in range(NDEV - 1):
        send(msgs.at[me], msgs.at[me], s_msg.at[0], m_msg.at[0], others[k])
    invl[...] = jnp.broadcast_to(1.0 / jnp.sum(acc, axis=1, keepdims=True), (ROWS, EMB))
    bcol[...] = jnp.broadcast_to((lq_own + shift) * LOG2E, (EMB, ROWS)).T

    p_own = diag[...] * jnp.exp2((c_own - crun[...]) * LOG2E) * invl[...]
    dacc[...] = dacc[...] * invl[...] + (p_own - 1.0).astype(BF16).astype(F32) * vall[me].astype(F32)
    gather_jobs(uall, 0, 1, s_u, m_u)

    def tower_backward(owner, x, w_out, a_ref, h_ref, u_ref, r_ref, g):
        d_unit = dacc[...] * GRAD_SCALE
        u = u_ref[...]
        de = (r_ref[...] * (d_unit - u * jnp.sum(u * d_unit, axis=-1, keepdims=True))).astype(BF16)
        g[2 * FEAT:PACK, :] = dot_tn(h_ref[...], de)
        hand_over(owner, g, GO)
        dh = dot_nt(de, w_out[...])
        da = jnp.where(a_ref[...] > 0, dh, 0.0).astype(BF16)
        gi = dot_tn(x[...], da)
        g[0:FEAT, :] = gi[:, 0:EMB]
        g[FEAT:2 * FEAT, :] = gi[:, EMB:HID]
        hand_over(owner, g, GI)

    bit = {1: bit_x, 2: bit_y, 4: bit_z}
    PLANE = ((0, 1), (1, 0), (1, 1))

    def slot(p, b0, b1, b2, count):
        eighth = SUM_ROWS[p] // 8
        return pl.ds(pl.multiple_of(SUM_BASE[p] + (b0 * 4 + b1 * 2 + b2) * eighth, 8), count * eighth)

    def part(p, share):
        return pl.ds(SUM_BASE[p] // share, SUM_ROWS[p] // share)

    def bits(p, flip=(0, 0)):
        b = [bit[d] for d in ORDERS[p]]
        return (b[0],) + tuple(1 - v if f else v for v, f in zip(b[1:], flip))

    def plane_dev(p, k):
        return dev(PLANE[k][0] * ORDERS[p][1] + PLANE[k][1] * ORDERS[p][2])

    def plane_shard(out, p, k):
        return out.at[slot(p, *bits(p, PLANE[k]), 1), :]

    def axis_half(out, p, far):
        b0 = bits(p)[0]
        return out.at[slot(p, 1 - b0 if far else b0, 0, 0, 4), :]

    GO, GI = pl.ds(2 * FEAT, HID), pl.ds(0, 2 * FEAT)

    def hand_over(owner, g, rows):
        @pl.when(core != owner)
        def _():
            send(g.at[rows, :], pp.at[rows, :], s_pair, m_pair, partner)

    def sum_pair(g):
        arrived(pp, m_pair)
        pp[...] = pp[...] + g[...]
        for p in range(3):
            send(pp.at[slot(p, 1 - bits(p)[0], 0, 0, 4), :], ra.at[part(p, 2), :], s_r1, m_r1, dev(ORDERS[p][0]))

    def sum_axis():
        arrived(ra, m_r1)
        for p in range(3):
            mine = slot(p, bits(p)[0], 0, 0, 4)
            pp[mine, :] = pp[mine, :] + ra[part(p, 2), :]
        for k in (2, 0, 1):
            for p in range(3):
                send(pp.at[slot(p, *bits(p, PLANE[k]), 1), :], rb.at[k, part(p, 8), :], s_r2, m_r2, plane_dev(p, k))

    def sum_plane(out):
        arrived(rb, m_r2)
        for p in range(3):
            total = pp[slot(p, *bits(p), 1), :]
            for k in range(3):
                total = total + rb[k, part(p, 8), :]
            fin[part(p, 8), :] = total
        for k in (2, 0, 1):
            for p in range(3):
                send(fin.at[part(p, 8), :], out.at[slot(p, *bits(p), 1), :], s_g1, m_g1.at[k], plane_dev(p, k))
        for p in range(3):
            place = out.at[slot(p, *bits(p), 1), :]
            send(fin.at[part(p, 8), :], place, s_g2, m_g2, dev(ORDERS[p][0]))
            pltpu.make_async_copy(fin.at[part(p, 8), :], place, s_own).start()

    def spread_plane(out):
        for k in range(3):
            arrived(fin, m_g1.at[k])
            for p in range(3):
                ref = plane_shard(out, p, k)
                send(ref, ref, s_g2, m_g2, dev(ORDERS[p][0]))
        pltpu.make_async_copy(fin, out.at[part(0, 1), :].at[0:HALF // 4, :], s_own).wait()
        for p in range(3):
            ref = axis_half(out, p, 0)
            send(ref, ref, s_fw, m_fw, partner)

    def spread_axis(out):
        arrived(ra, m_g2)
        for p in range(3):
            ref = axis_half(out, p, 1)
            send(ref, ref, s_fw, m_fw, partner)

    def on_core(owner, stage, *args):
        @pl.when(core == owner)
        def _():
            stage(*args)

    def dv_block(b, own=False):
        s = dot_nt(vall[me], uall[b])
        p = jnp.exp2(s * LOGIT_SCALE - wide(bcol[...])) * msgs[b, :, 0:ROWS]
        if own:
            p = jnp.where(eye, p - 1.0, p)
        return dot_nn(p.astype(BF16), uall[b])

    tower_backward(0, qx, wqo, a_q, h_q, u_q, r_q, gp_q)
    gather_jobs(uall, 0, 2, s_u, m_u)
    pair_send(uall, 1, s_u.at[1], m_ud)
    dacc[...] = dv_block(me, True)
    gather_jobs(uall, 1, 1, s_u, m_u)
    on_core(0, sum_pair, gp_q)

    arrived(msgs.at[0:NDEV - 1], m_msg.at[0])
    total = msgs[0, :, ROWS:MSG]
    for b in range(1, NDEV):
        total = total + msgs[b, :, ROWS:MSG]
    loss_out[...] = jnp.broadcast_to(jnp.sum(total, axis=1, keepdims=True) * (1.0 / TOTAL), (1, 128))

    def dv_group(blocks):
        total = dacc[...]
        for b in blocks:
            total = total + dv_block(b)
        dacc[...] = total

    def dv_step(g, _):
        @pl.when(g == 1)
        def _():
            gather_jobs(uall, 1, 2, s_u, m_u)
            pair_send(uall, 2, s_u.at[1], m_ud)
            pair_wait(uall, 1, m_ud)

        @pl.when(g == 2)
        def _():
            on_core(0, sum_axis)

        @pl.when(g == 3)
        def _():
            gather_jobs(uall, 2, 2, s_u, m_u)
            pair_send(uall, 3, s_u.at[1], m_ud)
            pair_wait(uall, 2, m_ud)

        @pl.when(g == 4)
        def _():
            pair_wait(uall, 3, m_ud)

        dv_group([nth_dev(3 * g + j) for j in range(3)])
        return 0

    pair_wait(uall, 0, m_ud)
    lax.fori_loop(0, 5, dv_step, 0)
    tower_backward(1, vx, wvo, a_v, h_v, u_v, r_v, gp_v)
    on_core(0, sum_plane, gq_out)
    sent(vall.at[0:7], s_v.at[0])
    sent(lqall.at[0:7], s_v.at[1])
    sent(vall.at[0:8], s_v.at[2])
    sent(lqall.at[0:8], s_v.at[3])
    sent(uall.at[0:7], s_u.at[0])
    sent(uall.at[0:8], s_u.at[1])
    sent(msgs.at[0:NDEV - 1], s_msg.at[0])
    on_core(1, sum_pair, gp_v)
    on_core(0, spread_plane, gq_out)
    on_core(1, sum_axis)
    on_core(0, spread_axis, gq_out)
    on_core(1, sum_plane, gv_out)
    on_core(1, spread_plane, gv_out)
    on_core(1, spread_axis, gv_out)
    sent(pp, s_pair)
    for like, ssem in ((ra, s_r1), (rb, s_r2), (rb, s_g1), (ra, s_g2), (pp, s_fw)):
        sent(like, ssem)
    arrived(pp, m_fw)


def finish(loss, gq, gv, loss_out, gqi, gqo, gvi, gvo, scalar, sem):
    scalar[0] = loss[0, 0]
    copies = [(scalar, loss_out)]
    for g, gi, go in ((gq, gqi, gqo), (gv, gvi, gvo)):
        copies += [(g.at[0:FEAT, :], gi.at[:, 0:EMB]), (g.at[FEAT:2 * FEAT, :], gi.at[:, EMB:HID]),
                   (g.at[2 * FEAT:PACK, :], go)]
    copies = [pltpu.make_async_copy(src, dst, sem.at[n]) for n, (src, dst) in enumerate(copies)]
    for copy in copies:
        copy.start()
    for copy in copies:
        copy.wait()


def solution(mesh):
    vmem = pl.BlockSpec(memory_space=pltpu.VMEM)
    hbm = pl.BlockSpec(memory_space=pltpu.HBM)
    anym = pl.BlockSpec(memory_space=pl.ANY)
    dma = pltpu.SemaphoreType.DMA
    V = pltpu.VMEM

    def local_step(query_feat, item_feat, log_q, w_query_in, w_query_out, w_item_in, w_item_out):
        shape = jax.ShapeDtypeStruct
        loss, gq, gv = pl.pallas_call(
            kernel,
            out_shape=(shape((1, 128), F32), shape((PACK, EMB), F32), shape((PACK, EMB), F32)),
            in_specs=[hbm] * 7,
            out_specs=(vmem, anym, anym),
            scratch_shapes=(
                [V((ROWS, FEAT), BF16)] * 2 + [V((FEAT, HID), BF16), V((HID, EMB), BF16)] * 2 + [dma((7,))]
                + [V((NDEV, ROWS, EMB), BF16)] * 2
                + [V((NDEV, 1, ROWS), F32), V((1, EMB), F32), V((1, ROWS), F32), V((NDEV, 1, MSG), F32)]
                + [V((ROWS, EMB), F32)] * 5
                + [V((ROWS, HID), F32)] * 2 + [V((ROWS, HID), BF16)] * 2 + [V((ROWS, EMB), F32)] * 4
                + [V((PACK, EMB), F32)] * 3 + [V((HALF, EMB), F32), V((3, HALF // 4, EMB), F32), V((HALF // 4, EMB), F32)]
                + [dma]
                + [dma((1,))] * 2 + [dma((n,)) for n in (4, 6, 8, 4, 4, 2, 6, 4)]
                + [dma] * 7 + [dma((3,))] + [dma] * 4),
            compiler_params=pltpu.CompilerParams(collective_id=0, has_side_effects=True,
                                                 vmem_limit_bytes=48 * 1024 * 1024),
            name="step",
        )(*(pltpu.with_memory_space_constraint(x, pltpu.HBM) for x in (
            query_feat, item_feat, log_q.reshape(1, ROWS), w_query_in, w_query_out, w_item_in, w_item_out)))
        return pl.pallas_call(
            finish,
            out_shape=(shape((1,), F32), shape((FEAT, HID), F32), shape((HID, EMB), F32),
                       shape((FEAT, HID), F32), shape((HID, EMB), F32)),
            in_specs=[vmem, anym, anym],
            out_specs=(hbm,) * 5,
            scratch_shapes=[pltpu.SMEM((1,), F32), dma((7,))],
            compiler_params=pltpu.CompilerParams(vmem_limit_bytes=8 * 1024 * 1024),
            name="finish",
        )(loss, gq, gv)

    return jax.shard_map(local_step, mesh=mesh, in_specs=(P('dp', None), P('dp', None), P('dp'), P(), P(), P(), P()), out_specs=(P(), P(), P(), P(), P()), check_vma=False)
```
